32 devices in a mesh: dp: 8 (over y, x, core), expert: 4 (over z).
Axes of the slice: x: 2, y: 2, z: 4, core: 2. Of those that a mesh axis runs over, the one named last changes fastest.
Arguments:
- tokens: bfloat16 [512, 2048], P('expert', 'dp'), may hold values from -6 to 6
- routes: int32 [512, 2], P('expert'), may hold values from 0 to 3, all different within a row
- dt_raw: float32 [512, 32], P('expert', 'dp'), may hold values from -5 to 5
- b_proj: float32 [512, 16], P('expert'), may hold values from -1.8 to 1.8
- c_proj: float32 [512, 16], P('expert'), may hold values from -1.8 to 1.8
- decay_rate: float32 [32], P('dp'), may hold values from 0.002 to 0.2
- skip_gain: float32 [32], P('dp'), may hold values from 0.5 to 1.5
- router_weight: float32 [2048, 4], P('dp'), may hold values from -0.125 to 0.125
- gate_weight: bfloat16 [4, 2048, 7168], P('expert', None, 'dp'), may hold values from -0.125 to 0.125
- up_weight: bfloat16 [4, 2048, 7168], P('expert', None, 'dp'), may hold values from -0.125 to 0.125
- down_weight: bfloat16 [4, 7168, 2048], P('expert', 'dp'), may hold values from -0.0625 to 0.0625
- out_grad: bfloat16 [512, 2048], P('expert', 'dp'), may hold values from -6 to 6
Outputs:
- block_out: bfloat16 [512, 2048], P('expert', 'dp')
- token_grad: bfloat16 [512, 2048], P('expert', 'dp')
- gate_grad: bfloat16 [4, 2048, 7168], P('expert', None, 'dp')
- up_grad: bfloat16 [4, 2048, 7168], P('expert', None, 'dp')
- down_grad: bfloat16 [4, 7168, 2048], P('expert', 'dp')
- router_grad: float32 [2048, 4], P('dp')
- rate_grad: float32 [32], P('dp')
- skip_grad: float32 [32], P('dp')
The draws below stay inside these ranges and needn't reach their ends.
Inputs may be any that keep to these rules, and one draw needn't show every extreme that they name: `routes`: each token names two different experts.
All inputs are finite; a program needn't handle non-finite values.
Results may differ from the reference program's by a relative error of at most 0.02.
Values may be sent and summed in bfloat16 or wider, within the bound.
A program may use at most 64 MiB of HBM per device.

```python
import math
import jax
import jax.numpy as jnp
from jax import lax

D = 2048
FF = 7168
HEAD_DIM = 64
STATE = 16
TOK_DEV = 128
CAP = 80
HEADS = 32
EXPERTS = 4
LENGTH = 512
N_DP = 8
N_EXPERT = 4


def shard_levels(rng, dims, cuts, least, largest):
    level, own = 1.0, jax.random.fold_in(rng, 6)
    for position, shards_of in cuts:
        draws = jnp.exp(jax.random.uniform(jax.random.fold_in(own, position), (shards_of,), jnp.float32, least / len(cuts), largest / len(cuts)))
        level = level * jnp.repeat(draws, dims[position] // shards_of).reshape([-1 if axis == position else 1 for axis in range(len(dims))])
    return level


def different_ones(rng, rows, amount, top, lift):
    order = jax.random.permutation(jax.random.fold_in(rng, 1), amount)
    favour = order
    for power in range(3):
        favour = favour * favour // amount
    favour = favour * lift // amount
    lots = jax.random.randint(jax.random.fold_in(rng, 2), (rows, amount), 0, 4096) + favour
    fixed_rows = jax.random.permutation(jax.random.fold_in(rng, 3), rows)[jnp.arange(amount) % rows]
    lots = jnp.where(jnp.arange(rows)[:, None] == fixed_rows[None, :], 1 << 14, lots)
    priority = lots * amount + jnp.arange(amount)
    return lax.top_k(priority.astype(jnp.int32), top)[1].astype(jnp.int32)


def normal_values(stream_key, dims, scale, bound, cuts=(), kind=jnp.bfloat16):
    loudness = shard_levels(stream_key, dims, cuts, -0.22, 0.18) if cuts else 1.0
    drawn = jax.random.normal(stream_key, dims, jnp.float32) * scale * loudness
    return jnp.minimum(jnp.maximum(drawn, -bound), bound).astype(kind)


def setup_inputs(seed: int = 0) -> dict:
    splits = jax.random.split(jax.random.key(seed), 13)
    tokens = normal_values(splits[0], (LENGTH, D), 1.0, 6.0, ((0, 4), (1, 8)))
    routes = different_ones(splits[1], LENGTH, EXPERTS, 2, 8192)
    dt_raw = normal_values(splits[2], (LENGTH, HEADS), 1.0, 5.0, ((0, 4), (1, 8)), jnp.float32)
    b_proj = normal_values(splits[3], (LENGTH, STATE), 0.3, 1.8, ((0, 4),), jnp.float32)
    c_proj = normal_values(splits[4], (LENGTH, STATE), 0.3, 1.8, ((0, 4),), jnp.float32)
    decay_rate = jnp.clip(jnp.exp(math.log(0.2) - 4.6051702 * jax.random.uniform(splits[5], (HEADS,), jnp.float32) ** shard_levels(splits[5], (HEADS,), ((0, 8),), -0.2, 0.2)), 0.002, 0.2)
    skip_gain = jnp.clip(0.5 + 1.0 * jax.random.uniform(splits[6], (HEADS,), jnp.float32) ** shard_levels(splits[6], (HEADS,), ((0, 8),), -0.2, 0.2), 0.5, 1.5)
    router_weight = normal_values(splits[7], (D, EXPERTS), D ** -0.5, 0.125, ((0, 8),), jnp.float32)
    gate_weight = normal_values(splits[8], (EXPERTS, D, FF), D ** -0.5, 0.125, ((0, 4), (2, 8)))
    up_weight = normal_values(splits[9], (EXPERTS, D, FF), D ** -0.5, 0.125, ((0, 4), (2, 8)))
    down_weight = normal_values(splits[10], (EXPERTS, FF, D), FF ** -0.5, 0.0625, ((0, 4), (1, 8)))
    out_grad = normal_values(splits[11], (LENGTH, D), 1.0, 6.0, ((0, 4), (1, 8)))
    return {"tokens": tokens, "routes": routes, "dt_raw": dt_raw, "b_proj": b_proj, "c_proj": c_proj, "decay_rate": decay_rate, "skip_gain": skip_gain, "router_weight": router_weight, "gate_weight": gate_weight, "up_weight": up_weight, "down_weight": down_weight, "out_grad": out_grad}


EPSILON = 1e-06
HIGHEST = lax.Precision.HIGHEST

def rms_norm(values):
    return values * lax.rsqrt(lax.optimization_barrier(jnp.mean(values * values, axis=-1, keepdims=True)) + EPSILON)

def end_parts(normed, b_rows, dt_rows, decay_rate):
    steps_total = normed.shape[0]
    head_count = decay_rate.shape[0]
    step_size = jax.nn.softplus(dt_rows)
    running = jnp.cumsum(-step_size * decay_rate[None, :], axis=0)
    tail_weight = jnp.exp(running[-1][None, :] - running) * step_size
    head_rows = normed.reshape(steps_total, head_count, -1)
    local_state = jnp.einsum('sh,shp,sn->hpn', tail_weight, head_rows, b_rows, precision=HIGHEST)
    return (jnp.exp(running[-1]), local_state.reshape(head_count, -1))

def ssd_piece(normed, b_rows, c_rows, dt_rows, decay_rate, skip_gain, state_start):
    steps_total = normed.shape[0]
    head_count = decay_rate.shape[0]
    state_width = b_rows.shape[1]
    step_size = jax.nn.softplus(dt_rows)
    running = jnp.cumsum(-step_size * decay_rate[None, :], axis=0)
    positions = jnp.arange(steps_total, dtype=jnp.int32)
    causal = (positions[:, None] >= positions[None, :])[:, :, None]
    spread = jnp.where(causal, running[:, None, :] - running[None, :, :], 0.0)
    decay_table = jnp.where(causal, jnp.exp(spread), 0.0)
    pairing = jnp.dot(c_rows, b_rows.T, precision=HIGHEST)
    mixing = decay_table * pairing[:, :, None] * step_size[None, :, :]
    head_rows = normed.reshape(steps_total, head_count, -1)
    state_three = state_start.reshape(head_count, -1, state_width)
    mixed = jnp.einsum('tsh,shp->thp', mixing, head_rows, precision=HIGHEST)
    mixed = mixed + jnp.einsum('tn,th,hpn->thp', c_rows, jnp.exp(running), state_three, precision=HIGHEST)
    mixed = mixed + skip_gain[None, :, None] * head_rows
    decay_total, local_state = end_parts(normed, b_rows, dt_rows, decay_rate)
    state_end = decay_total[:, None] * state_start + local_state
    return (mixed.reshape(steps_total, -1), state_end)

def dispatch_table(choice_ids, expert_count, capacity):
    flat_ids = choice_ids.reshape(-1)
    row_total = flat_ids.shape[0]
    expert_hot = (flat_ids[:, None] == jnp.arange(expert_count, dtype=jnp.int32)[None, :]).astype(jnp.float32)
    positions = jnp.arange(row_total, dtype=jnp.int32)
    lower = (positions[:, None] > positions[None, :]).astype(jnp.float32)
    earlier = jnp.dot(lower, expert_hot, precision=HIGHEST)
    slot_index = lax.optimization_barrier(jnp.sum(earlier * expert_hot, axis=1))
    target = flat_ids.astype(jnp.float32) * capacity + slot_index
    target = jnp.where(slot_index < capacity, target, -1.0)
    slot_ids = jnp.arange(expert_count * capacity, dtype=jnp.int32).astype(jnp.float32)
    return (slot_ids[:, None] == target[None, :]).astype(jnp.float32)

def block_sum(parts):
    rounded = lax.optimization_barrier(parts.astype(jnp.bfloat16))
    return lax.optimization_barrier(jnp.sum(rounded.astype(jnp.float32), axis=1)).astype(jnp.bfloat16)

def reference(tokens, routes, dt_raw, b_proj, c_proj, decay_rate, skip_gain, router_weight, gate_weight, up_weight, down_weight, out_grad):
    blocks = N_EXPERT
    unit_size = FF // N_DP
    inputs = tokens.astype(jnp.float32)

    def mixer_all(inputs_in, rate_in, skip_in):
        normed = rms_norm(inputs_in).reshape(blocks, TOK_DEV, D)

        def one_block(state, pieces):
            normed_rows, b_rows, c_rows, dt_rows = pieces
            mixed_rows, state_end = ssd_piece(normed_rows, b_rows, c_rows, dt_rows, rate_in, skip_in, state)
            return (state_end, mixed_rows)
        zero_state = jnp.zeros((HEADS, HEAD_DIM * STATE), jnp.float32)
        final_state, mixed_all = lax.scan(one_block, zero_state, (normed, b_proj.reshape(blocks, TOK_DEV, STATE), c_proj.reshape(blocks, TOK_DEV, STATE), dt_raw.reshape(blocks, TOK_DEV, HEADS)))
        return mixed_all.reshape(LENGTH, D)
    mixed, mixer_pull = jax.vjp(mixer_all, inputs, decay_rate, skip_gain)
    resid = (inputs + mixed).astype(jnp.bfloat16)
    resid_f = resid.astype(jnp.float32).reshape(blocks, TOK_DEV, D)
    pre_moe, norm_pull = jax.vjp(rms_norm, resid_f)
    moe_in = pre_moe.astype(jnp.bfloat16)
    moe_f = moe_in.astype(jnp.float32)
    choice_ids = routes.reshape(blocks, TOK_DEV, 2)
    logits = jnp.einsum('btd,de->bte', moe_f, router_weight, precision=HIGHEST)
    expert_ids = jnp.arange(EXPERTS, dtype=jnp.int32)
    first_hot = (choice_ids[:, :, 0:1] == expert_ids).astype(jnp.float32)
    second_hot = (choice_ids[:, :, 1:2] == expert_ids).astype(jnp.float32)
    logit_gap = lax.optimization_barrier(jnp.sum(logits * (first_hot - second_hot), axis=2))
    first_weight = jax.nn.sigmoid(logit_gap)
    second_weight = jax.nn.sigmoid(-logit_gap)
    tables = jax.vmap(lambda ids_block: dispatch_table(ids_block, EXPERTS, CAP))(choice_ids)
    doubled = jnp.repeat(moe_f, 2, axis=1)
    send_rows = jnp.einsum('bsp,bpd->bsd', tables, doubled, precision=HIGHEST).astype(jnp.bfloat16)

    def to_experts(rows):
        shaped = rows.reshape(N_EXPERT, EXPERTS, CAP, D)
        return shaped.transpose(1, 0, 2, 3).reshape(EXPERTS, blocks * CAP, D)

    def from_experts(rows):
        shaped = rows.reshape(EXPERTS, N_EXPERT, CAP, D)
        return shaped.transpose(1, 0, 2, 3).reshape(blocks, EXPERTS * CAP, D)
    expert_rows = to_experts(send_rows)

    def expert_forward(pieces):
        rows, gate_w, up_w, down_w = pieces
        gate_pre = jnp.dot(rows, gate_w, preferred_element_type=jnp.float32)
        up_pre = jnp.dot(rows, up_w, preferred_element_type=jnp.float32)
        hidden = (jax.nn.silu(gate_pre) * up_pre).astype(jnp.bfloat16)
        parts = jnp.einsum('rbf,bfd->rbd', hidden.astype(jnp.float32).reshape(-1, N_DP, unit_size), down_w.astype(jnp.float32).reshape(N_DP, unit_size, D), precision=HIGHEST)
        return block_sum(parts)
    expert_out = lax.map(expert_forward, (expert_rows, gate_weight, up_weight, down_weight))
    back_rows = from_experts(expert_out).astype(jnp.float32)
    per_slot = jnp.einsum('bsp,bsd->bpd', tables, back_rows, precision=HIGHEST).reshape(blocks, TOK_DEV, 2, D)
    moe_sum = first_weight[:, :, None] * per_slot[:, :, 0] + second_weight[:, :, None] * per_slot[:, :, 1]
    block_out = (resid_f + moe_sum).astype(jnp.bfloat16).reshape(LENGTH, D)
    upstream = out_grad.astype(jnp.float32).reshape(blocks, TOK_DEV, D)
    first_back = lax.optimization_barrier(jnp.sum(upstream * per_slot[:, :, 0], axis=2))
    second_back = lax.optimization_barrier(jnp.sum(upstream * per_slot[:, :, 1], axis=2))
    slot_grad = jnp.stack([first_weight[:, :, None] * upstream, second_weight[:, :, None] * upstream], axis=2)
    slot_grad = slot_grad.reshape(blocks, 2 * TOK_DEV, D).astype(jnp.bfloat16)
    grad_send = jnp.einsum('bsp,bpd->bsd', tables, slot_grad.astype(jnp.float32), precision=HIGHEST).astype(jnp.bfloat16)
    grad_rows_all = to_experts(grad_send)

    def expert_backward(pieces):
        rows, grad_rows, gate_w, up_w, down_w = pieces
        gate_pre = jnp.dot(rows, gate_w, preferred_element_type=jnp.float32)
        up_pre = jnp.dot(rows, up_w, preferred_element_type=jnp.float32)
        hidden = (jax.nn.silu(gate_pre) * up_pre).astype(jnp.bfloat16)
        unit_grad = lax.dot_general(grad_rows, down_w, (((1,), (1,)), ((), ())), preferred_element_type=jnp.float32)
        sigma = jax.nn.sigmoid(gate_pre)
        gate_back = (unit_grad * up_pre * sigma * (1.0 + gate_pre * (1.0 - sigma))).astype(jnp.bfloat16)
        up_back = (unit_grad * jax.nn.silu(gate_pre)).astype(jnp.bfloat16)
        down_part = lax.dot_general(hidden, grad_rows, (((0,), (0,)), ((), ())), preferred_element_type=jnp.float32)
        gate_part = lax.dot_general(rows, gate_back, (((0,), (0,)), ((), ())), preferred_element_type=jnp.float32)
        up_part = lax.dot_general(rows, up_back, (((0,), (0,)), ((), ())), preferred_element_type=jnp.float32)
        parts = jnp.einsum('rbf,dbf->rbd', gate_back.astype(jnp.float32).reshape(-1, N_DP, unit_size), gate_w.astype(jnp.float32).reshape(D, N_DP, unit_size), precision=HIGHEST)
        parts = parts + jnp.einsum('rbf,dbf->rbd', up_back.astype(jnp.float32).reshape(-1, N_DP, unit_size), up_w.astype(jnp.float32).reshape(D, N_DP, unit_size), precision=HIGHEST)
        return (block_sum(parts), gate_part.astype(jnp.bfloat16), up_part.astype(jnp.bfloat16), down_part.astype(jnp.bfloat16))
    input_back, gate_grad, up_grad, down_grad = lax.map(expert_backward, (expert_rows, grad_rows_all, gate_weight, up_weight, down_weight))
    returned = from_experts(input_back).astype(jnp.float32)
    slot_back = jnp.einsum('bsp,bsd->bpd', tables, returned, precision=HIGHEST).reshape(blocks, TOK_DEV, 2, D)
    moe_grad = slot_back[:, :, 0] + slot_back[:, :, 1]
    gap_grad = first_weight * second_weight * (first_back - second_back)
    logit_grad = gap_grad[:, :, None] * (first_hot - second_hot)
    moe_in_grad = moe_grad + jnp.einsum('bte,de->btd', logit_grad, router_weight, precision=HIGHEST)
    router_grad = jnp.einsum('btd,bte->de', moe_f, logit_grad, precision=HIGHEST)
    resid_grad = upstream + norm_pull(moe_in_grad)[0]
    resid_grad = resid_grad.reshape(LENGTH, D)
    mixer_input_grad, rate_grad, skip_grad = mixer_pull(resid_grad)
    token_grad = (resid_grad + mixer_input_grad).astype(jnp.bfloat16)
    return (block_out, token_grad, gate_grad, up_grad, down_grad, router_grad, rate_grad, skip_grad)
```

```python
import functools
import types
import jax
import jax.numpy as jnp
from jax import lax
from jax.experimental import pallas as pl
from jax.experimental.pallas import tpu as pltpu
from jax.sharding import PartitionSpec as P


EPSILON = 1e-06
HIGHEST = lax.Precision.HIGHEST
MESH = pl.DeviceIdType.MESH
DP, EXPERT = ("dp", "expert")
SEND, RECV, SRC, ALL = ("_send", "_recv", "_src", "_all")
HALF, FULL = (jnp.bfloat16, jnp.float32)
NN = (((1,), (0,)), ((), ()))
NT = (((1,), (1,)), ((), ()))
TN = (((0,), (0,)), ((), ()))


def loop(count, step):
    def run(i, carry):
        step(i)
        return carry

    lax.fori_loop(0, count, run, 0)


def slices(total, width):
    return [(at, min(width, total - at)) for at in range(0, total, width)]


def exact(a, b, dims=NN):
    return lax.dot_general(a, b, dims, precision=HIGHEST, preferred_element_type=FULL)


def fast(a, b, dims=NN):
    return lax.dot_general(a, b, dims, preferred_element_type=FULL)


def iota(shape, axis):
    return lax.broadcasted_iota(jnp.int32, shape, axis)


def softplus(v):
    return jnp.maximum(v, 0.0) + jnp.log(1.0 + jnp.exp(-jnp.abs(v)))


def sigmoid(v):
    return 1.0 / (1.0 + jnp.exp(-v))


def step_kernel(names, capacity, cap, fused, *refs):
    r = types.SimpleNamespace(**dict(zip(names, refs)))
    peers, place = (lax.axis_size(DP), lax.axis_index(DP))
    blocks, block = (lax.axis_size(EXPERT), lax.axis_index(EXPERT))
    chip_count = peers // 2
    chip, core = (place // 2, lax.rem(place, 2))
    partner = place + 1 - 2 * core
    count, width = r.tokens.shape
    features = width * peers
    heads = r.dt.shape[0]
    head_dim = width // heads
    experts = r.router.shape[0]
    units = r.down_w.shape[0]
    total = blocks * cap
    stat_rows = r.stat_src.shape[0]
    rows, grads = (r.rows, r.grads)
    sources, wholes = ((r.send_rows, r.send_grads), (rows, grads))
    away, mine, pair, chips = (r.away, r.mine, r.pair, r.chips)
    summed = r.summed
    backs = (r.back_f, r.back_b)
    down_w = r.down_w

    def strip(j):
        return pl.ds(pl.multiple_of(j * cap, 16), cap)

    def columns(d):
        return pl.ds(pl.multiple_of(d * width, 128), width)

    def ahead(k):
        return lax.rem(block + k, blocks)

    def origin_of(k):
        return lax.rem(block + blocks - k, blocks)

    def chip_at(q):
        return lax.rem(chip + q, chip_count)

    def chip_from(q):
        return lax.rem(chip + chip_count - q, chip_count)

    if fused:
        gu_w, gu_s = ((r.gu_w,), (r.gu_s,))
        gu_back, gu_back2 = ((r.gu_back,), (r.gu_back2,))
        halves = (r.gu_w.at[:, :units], r.gu_w.at[:, units:])

        def part(group, which, row, at, span):
            lo = at + which * units
            return group[0].at[row, lo : lo + span]
    else:
        gu_w, gu_s = ((r.gate_w, r.up_w), (r.gate_s, r.up_s))
        gu_back = (r.gate_back, r.up_back)
        gu_back2 = (r.gate_back2, r.up_back2)
        halves = (r.gate_w, r.up_w)

        def part(group, which, row, at, span):
            return group[which].at[row, at : at + span]

    weights = [
        pltpu.make_async_copy(hbm.at[0], held, r.weight_sem.at[n])
        for n, (hbm, held) in enumerate(
            ((r.down_hbm, down_w), (r.gate_hbm, halves[0]), (r.up_hbm, halves[1]))
        )
    ]
    for item in weights:
        item.start()

    barrier = pltpu.get_barrier_semaphore()
    for axis, amount, me in ((DP, peers, place), (EXPERT, blocks, block)):

        def signal(k):
            pl.semaphore_signal(
                barrier, 1, device_id={axis: lax.rem(me + k + 1, amount)}, device_id_type=MESH
            )

        loop(amount - 1, signal)

    def exchange(axis, src, land, sems):
        amount, me = (peers, place) if axis == DP else (blocks, block)
        send, recv = (getattr(r, sems + SEND), getattr(r, sems + RECV))

        def copy(k, at):
            return pltpu.make_async_remote_copy(
                src_ref=src(lax.rem(me + k, amount)),
                dst_ref=land(at),
                send_sem=send.at[k],
                recv_sem=recv.at[k],
                device_id={axis: lax.rem(me + k, amount)},
                device_id_type=MESH,
            )

        def start():
            loop(amount - 1, lambda k: copy(k + 1, me).start())

        def arrive():
            loop(
                amount - 1,
                lambda k: copy(k + 1, lax.rem(me + amount - k - 1, amount)).wait_recv(),
            )

        def sent():
            loop(amount - 1, lambda k: copy(k + 1, me).wait_send())

        return start, arrive, sent

    def shared(axis, name):
        src, everyone = (getattr(r, name + SRC), getattr(r, name + ALL))
        start, arrive, sent = exchange(
            axis, lambda _: src, lambda at: everyone.at[at], name
        )

        def launch(value):
            src[...] = value
            start()
            everyone[place if axis == DP else block] = value

        return launch, arrive, sent

    square_launch, square_arrive, square_sent = shared(DP, "square")
    decay_launch, decay_arrive, decay_sent = shared(EXPERT, "decay")
    state_launch, state_arrive, state_sent = shared(EXPERT, "state")
    stat_launch, stat_arrive, stat_sent = shared(DP, "stat")
    inner_launch, inner_arrive, inner_sent = shared(DP, "inner")
    sgrad_launch, sgrad_arrive, sgrad_sent = shared(EXPERT, "sgrad")
    router_launch, router_arrive, router_sent = shared(EXPERT, "rout")
    last_launch, last_arrive, last_sent = shared(DP, "last")
    small_launch, small_arrive, small_sent = shared(EXPERT, "small")
    slot_start, slot_arrive, slot_sent = exchange(
        EXPERT, lambda to: r.slot_src.at[to], lambda at: r.slot_all.at[at], "slot"
    )
    value_start, value_arrive, value_sent = exchange(
        EXPERT, lambda to: r.value_src.at[to], lambda at: r.value_all.at[at], "value"
    )

    def own_copy(t):
        return pltpu.make_async_copy(
            sources[t].at[strip(block), :],
            wholes[t].at[strip(block), columns(place)],
            r.local_sem.at[t],
        )

    def z_copy(t, k, land):
        return pltpu.make_async_remote_copy(
            src_ref=sources[t].at[strip(ahead(k)), :],
            dst_ref=wholes[t].at[strip(land), columns(place)],
            send_sem=r.z_send.at[t, k],
            recv_sem=r.z_recv.at[t, k],
            device_id={EXPERT: ahead(k)},
            device_id_type=MESH,
        )

    def spread_copy(t, k, j, q, owner):
        cut = wholes[t].at[strip(j), columns(owner)]
        return pltpu.make_async_remote_copy(
            src_ref=cut,
            dst_ref=cut,
            send_sem=r.c_send.at[t, k * chip_count + q],
            recv_sem=r.c_recv.at[t, k * chip_count + q],
            device_id={DP: 2 * chip_at(q) + core},
            device_id_type=MESH,
        )

    def partner_copy(t, k, j, q, owner):
        cut = wholes[t].at[strip(j), columns(owner)]
        return pltpu.make_async_remote_copy(
            src_ref=cut,
            dst_ref=cut,
            send_sem=r.p_send.at[t, k * chip_count + q],
            recv_sem=r.p_recv.at[t, k * chip_count + q],
            device_id={DP: partner},
            device_id_type=MESH,
        )

    def dispatch(t):
        own_copy(t).start()
        loop(blocks - 1, lambda k: z_copy(t, k + 1, block).start())

    def forward(t, k, j):
        loop(chip_count - 1, lambda q: spread_copy(t, k, j, q + 1, place).start())
        partner_copy(t, k, j, 0, place).start()

    def forward_own(t):
        own_copy(t).wait()
        forward(t, 0, block)

    def pass_on(t):
        def one(n):
            z_copy(t, n + 1, origin_of(n + 1)).wait_recv()
            forward(t, n + 1, origin_of(n + 1))

        loop(blocks - 1, one)

    def from_chip(t, q):
        owner = 2 * chip_from(q) + core

        def one(k):
            spread_copy(t, k, origin_of(k), q, owner).wait_recv()
            partner_copy(t, k, origin_of(k), q, owner).start()

        loop(blocks, one)

    def from_partner(t, q):
        owner = 2 * chip_from(q) + 1 - core
        loop(
            blocks, lambda k: partner_copy(t, k, origin_of(k), q, owner).wait_recv()
        )

    def pair_copy(t, c):
        return pltpu.make_async_remote_copy(
            src_ref=away.at[t, c],
            dst_ref=pair.at[t, c],
            send_sem=r.pair_send.at[t, c],
            recv_sem=r.pair_recv.at[t, c],
            device_id={DP: partner},
            device_id_type=MESH,
        )

    def chip_copy(t, q):
        return pltpu.make_async_remote_copy(
            src_ref=mine.at[t, chip_at(q)],
            dst_ref=chips.at[t, q],
            send_sem=r.chip_send.at[t, q],
            recv_sem=r.chip_recv.at[t, q],
            device_id={DP: 2 * chip_at(q) + core},
            device_id_type=MESH,
        )

    def back_copy(t, k, land):
        return pltpu.make_async_remote_copy(
            src_ref=summed.at[t, strip(ahead(k)), :],
            dst_ref=backs[t].at[strip(land), :],
            send_sem=r.back_send.at[t, k],
            recv_sem=r.back_recv.at[t, k],
            device_id={EXPERT: ahead(k)},
            device_id_type=MESH,
        )

    def tiles(t, term):
        def step(q):
            @pl.when(q < chip_count)
            def _():
                c = chip_at(lax.rem(q + 1, chip_count))
                away[t, c] = term(2 * c + 1 - core).astype(HALF)
                pair_copy(t, c).start()

            @pl.when(q > 0)
            def _():
                c = chip_at(lax.rem(q, chip_count))
                value = term(2 * c + core)
                pair_copy(t, c).wait_recv()
                mine[t, c] = (value + pair[t, c].astype(FULL)).astype(HALF)

                @pl.when(q < chip_count)
                def _():
                    chip_copy(t, q).start()

        loop(chip_count + 1, step)

    def finish(t):
        value = mine[t, chip].astype(FULL)
        for q in range(1, chip_count):
            chip_copy(t, q).wait_recv()
            value = value + chips[t, q].astype(FULL)
        summed[t] = value.astype(HALF)
        loop(blocks - 1, lambda k: back_copy(t, k + 1, block).start())
        backs[t][strip(block), :] = summed[t, strip(block), :]

    def backs_arrive(t):
        loop(
            blocks - 1, lambda n: back_copy(t, n + 1, origin_of(n + 1)).wait_recv()
        )

    inputs = r.tokens[...].astype(FULL)
    lane_head = iota((1, width), 1) // head_dim

    def spread_heads(cols):
        wide = jnp.zeros((cols.shape[0], width), FULL)
        for h in range(heads):
            wide = jnp.where(lane_head == h, cols[:, h : h + 1], wide)
        return wide

    ones_row = jnp.ones((8, width), FULL)
    square_part = exact(ones_row, inputs * inputs, NT)
    eye8 = (iota((8, 128), 0) == iota((8, 128), 1)).astype(FULL)
    eye_count = (iota((count, count), 0) == iota((count, count), 1)).astype(FULL)

    def to_columns(rows8):
        return exact(rows8, eye8, TN)

    pl.semaphore_wait(barrier, peers + blocks - 2)
    square_launch(square_part)

    routes_row = r.routes[...].astype(FULL)
    routes = exact(eye_count, routes_row, NT)
    expert_row = iota((stat_rows, count), 0).astype(FULL) - 1.0
    first_row = (routes_row[0:1, :] == expert_row).astype(FULL)
    second_row = (routes_row[1:2, :] == expert_row).astype(FULL)
    hot_gap_row = first_row - second_row
    expert_col = iota((count, experts), 1).astype(FULL)
    first_col = (routes[:, 0:1] == expert_col).astype(FULL)
    second_col = (routes[:, 1:2] == expert_col).astype(FULL)
    below = iota((count, count), 0) > iota((count, count), 1)
    above = (iota((count, count), 0) < iota((count, count), 1)).astype(HALF)
    earlier_row = fast((first_row + second_row).astype(HALF), above)
    earlier_col = fast(below.astype(HALF), (first_col + second_col).astype(HALF))

    def slot_of(earlier, hot, ids, axis):
        index = jnp.sum(earlier * hot, axis=axis, keepdims=True)
        return jnp.where(index < capacity, ids * cap + index, -1.0)

    slots_down = iota((total, count), 0).astype(FULL)
    slots_across = iota((count, total), 1).astype(FULL)
    first_table = slots_down == slot_of(earlier_row, first_row, routes_row[0:1, :], 0)
    second_table = slots_down == slot_of(earlier_row, second_row, routes_row[1:2, :], 0)
    first_back = slots_across == slot_of(earlier_col, first_col, routes[:, 0:1], 1)
    second_back = slots_across == slot_of(earlier_col, second_col, routes[:, 1:2], 1)
    either = (first_table | second_table).astype(HALF)
    r.table[:, :count] = first_table.astype(FULL)
    r.table[:, count:] = second_table.astype(FULL)
    r.across[:count, :] = first_back.astype(HALF)
    r.across[count:, :] = second_back.astype(HALF)

    r.send_grads[...] = fast(either, r.out_grad[...]).astype(HALF)
    dispatch(1)

    step_row = softplus(r.dt[...])
    step_col = exact(eye_count, step_row, NT)
    rate = r.rate[...]
    reached = jnp.where(below, 1.0, eye_count)
    sum_col = exact(reached, step_col)
    sum_row = exact(step_row, reached, NT)
    run_col = -sum_col * rate
    decay_end = jnp.exp(run_col[count - 1 : count, :])
    decay_wide = spread_heads(decay_end)
    decay_launch(jnp.broadcast_to(decay_wide, (8, width)))
    tail_col = jnp.exp(run_col[count - 1 : count, :] - run_col) * step_col
    tail_wide = spread_heads(tail_col)
    grow_wide = spread_heads(jnp.exp(run_col))
    skip_wide = spread_heads(r.skip[...])
    sum_wide = spread_heads(sum_col)
    b_side, c_side = (r.b_proj[...], r.c_proj[...])
    forward_own(1)

    square_arrive()
    scale_row_one = lax.rsqrt(jnp.sum(r.square_all[...], axis=0) / features + EPSILON)
    scale_one = to_columns(scale_row_one)[:, 0:1]
    normed = inputs * scale_one
    r.normed[...] = normed
    state_launch(exact(b_side, tail_wide * normed))

    causal = iota((count, count), 0) >= iota((count, count), 1)
    pairing = exact(c_side, b_side, TN)
    for h in range(heads):
        fall = run_col[:, h : h + 1] + sum_row[h : h + 1, :] * rate[0:1, h : h + 1]
        table = jnp.where(causal, jnp.exp(jnp.where(causal, fall, 0.0)), 0.0)
        r.mixing[:, h * count : (h + 1) * count] = table * pairing * step_row[h : h + 1, :]
        r.stack[h * count : (h + 1) * count, :] = jnp.where(lane_head == h, normed, 0.0)
    r.local[...] = exact(r.mixing[...], r.stack[...]) + skip_wide * normed
    pass_on(1)

    decay_arrive()
    state_arrive()

    def carry(states, reverse):
        held = jnp.zeros(r.state_src.shape, FULL)
        for k in range(blocks):
            at = blocks - 1 - k if reverse else k
            reach = at > block if reverse else at < block
            held = jnp.where(reach, r.decay_all[at][0:1, :] * held + states[at], held)
        return held

    state_in = carry(r.state_all, False)
    carried = grow_wide * exact(c_side, state_in, TN)
    r.carried[...] = carried
    resid = (inputs + (r.local[...] + carried)).astype(HALF)
    r.resid[...] = resid
    r.send_rows[...] = fast(either, resid).astype(HALF)
    dispatch(0)
    resid_f = resid.astype(FULL)
    eye_router = (iota((stat_rows, 128), 0) == iota((stat_rows, 128), 1) + 1).astype(FULL)
    router = r.router[...]
    router_row = exact(eye_router[:, :experts], router)
    squares = exact(ones_row[0:1], resid_f * resid_f, NT)
    stat_part = exact(router_row, resid_f, NT)
    stat_launch(jnp.where(iota((stat_rows, count), 0) == 0, squares, stat_part))
    forward_own(0)
    for q in range(1, chip_count):
        from_chip(1, q)

    stat_arrive()
    stats = jnp.sum(r.stat_all[...], axis=0)
    scale_row = lax.rsqrt(stats[0:1] / features + EPSILON)
    raw_gap = jnp.sum(stats * hot_gap_row, axis=0, keepdims=True)
    first_weight = sigmoid(raw_gap * scale_row)
    second_weight = sigmoid(-raw_gap * scale_row)
    pick8 = iota((8, 2 * count), 0)
    slot_rows = jnp.where(pick8 == 0, jnp.concatenate([first_weight, second_weight], axis=1), 0.0)
    slot_rows = jnp.where(pick8 == 1, jnp.concatenate([scale_row, scale_row], axis=1), slot_rows)
    r.slot_src[...] = jnp.zeros_like(r.slot_src)

    def fill_slot(e):
        r.slot_src[e, :, :cap] = exact(slot_rows, r.table[strip(e), :], NT)

    loop(blocks, fill_slot)
    slot_start()
    r.slot_all[block] = r.slot_src[block]
    pass_on(0)

    for q in range(chip_count):
        from_partner(1, q)
    weights[0].wait()
    for at, span in slices(units, 256):
        r.unit_raw[:, at : at + span] = fast(grads[...], down_w[at : at + span, :], NT)

    slot_arrive()
    pick = (iota((8, 256), 0) == iota((8, 256), 1) // 128).astype(FULL)

    def take_slots(j):
        wide = exact(r.slot_all[j], pick, TN)
        r.slot_weight[strip(j), :] = wide[:cap, :128]
        r.slot_scale[strip(j), :] = wide[:cap, 128:]

    loop(blocks, take_slots)

    weights[1].wait()
    weights[2].wait()
    for held in gu_s:
        held[...] = jnp.zeros_like(held)

    def chunk(d):
        for held, weight in zip(gu_s, gu_w):
            held[...] += fast(rows[:, columns(d)], weight[columns(d), :])

    def same_core(q):
        @pl.when(q > 0)
        def _():
            from_chip(0, q)

        chunk(2 * chip_from(q) + core)

    loop(chip_count, same_core)

    def other_core(q):
        from_partner(0, q)
        chunk(2 * chip_from(q) + 1 - core)

    loop(chip_count, other_core)

    tall = 16
    r.values[...] = jnp.zeros_like(r.values)

    def some_rows(i):
        row = pl.ds(pl.multiple_of(i * tall, tall), tall)
        scale = r.slot_scale[row, 0:1]
        weight = r.slot_weight[row, 0:1]
        first = jnp.zeros((tall, 1), FULL)
        second = jnp.zeros((tall, 1), FULL)
        for at, span in slices(units, 256):
            gate_raw = part(gu_s, 0, row, at, span)[...]
            up_raw = part(gu_s, 1, row, at, span)[...]
            unit_raw = r.unit_raw[row, at : at + span]
            gate, up = (gate_raw * scale, up_raw * scale)
            sigma = sigmoid(gate)
            silu = gate * sigma
            hid = silu * up
            unit = unit_raw * weight
            gate_b = unit * up * (sigma * (1.0 + gate * (1.0 - sigma)))
            up_b = unit * silu
            r.hidden[row, at : at + span] = hid.astype(HALF)
            r.hidden2[row, at : at + span] = (hid * weight).astype(HALF)
            part(gu_back, 0, row, at, span)[...] = gate_b.astype(HALF)
            part(gu_back, 1, row, at, span)[...] = up_b.astype(HALF)
            part(gu_back2, 0, row, at, span)[...] = (gate_b * scale).astype(HALF)
            part(gu_back2, 1, row, at, span)[...] = (up_b * scale).astype(HALF)
            first = first + jnp.sum(hid * unit_raw, axis=1, keepdims=True)
            second = second + jnp.sum(gate_b * gate_raw + up_b * up_raw, axis=1, keepdims=True)
        lanes = iota((tall, 128), 1)
        r.values[row, :] = jnp.where(lanes == 0, first, jnp.where(lanes == 1, second, 0.0))

    loop(total // tall, some_rows)
    r.value_src[...] = jnp.zeros_like(r.value_src)

    def fill_value(j):
        r.value_src[j, :, :cap] = exact(eye8, r.values[strip(j), :], NT)

    loop(blocks, fill_value)
    value_start()
    r.value_all[block] = r.value_src[block]

    def input_term(d):
        result = None
        for back, weight in zip(gu_back, gu_w):
            term = fast(back[...], weight[columns(d), :], NT)
            result = term if result is None else result + term
        return result

    def output_term(d):
        return fast(r.hidden[...], down_w[:, columns(d)])

    tiles(1, input_term)

    value_arrive()

    def add_values(j, kept):
        return kept + exact(r.value_all[j, :, :cap], r.table[strip(j), :])

    inner_part = lax.fori_loop(0, blocks, add_values, jnp.zeros((8, 2 * count), FULL))
    inner_launch(inner_part)

    tiles(0, output_term)

    wide_cut = 256

    def weight_grads(lo, hi):
        def one(i):
            at = pl.ds(pl.multiple_of(i * wide_cut, wide_cut), wide_cut)
            if fused:
                value = fast(rows[:, at], gu_back2[0][...], TN)
                r.gate_grad[at, :] = value[:, :units].astype(HALF)
                r.up_grad[at, :] = value[:, units:].astype(HALF)
            else:
                r.gate_grad[at, :] = fast(rows[:, at], gu_back2[0][...], TN).astype(HALF)
                r.up_grad[at, :] = fast(rows[:, at], gu_back2[1][...], TN).astype(HALF)

        lax.fori_loop(lo, hi, lambda i, c: (one(i), c)[1], 0)

    def down_grads(lo, hi):
        for at, span in slices(units, 256)[lo:hi]:
            r.down_grad[at : at + span, :] = fast(
                r.hidden2[:, at : at + span], grads[...], TN
            ).astype(HALF)

    cuts = features // wide_cut
    down_cuts = len(slices(units, 256))
    weight_grads(0, cuts // 2)

    inner_arrive()
    inner_all = jnp.sum(r.inner_all[...], axis=0)
    gap_grad = first_weight * second_weight * (inner_all[0:1, :count] - inner_all[0:1, count:])
    inner_row = inner_all[1:2, :count] + inner_all[1:2, count:] + gap_grad * raw_gap
    row8 = iota((8, count), 0)
    packed = jnp.where(row8 == 0, scale_row, 0.0)
    packed = jnp.where(row8 == 1, inner_row, packed)
    packed = jnp.where(row8 == 2, gap_grad, packed)
    packed = jnp.where(row8 == 3, first_weight, packed)
    packed = jnp.where(row8 == 4, second_weight, packed)
    packed_cols = to_columns(packed)
    scale_two, inner_col = (packed_cols[:, 0:1], packed_cols[:, 1:2])
    gap_col = packed_cols[:, 2:3]
    weight_one, weight_two = (packed_cols[:, 3:4], packed_cols[:, 4:5])
    resid_f = r.resid[...].astype(FULL)
    router_launch(exact(gap_grad * hot_gap_row, resid_f * scale_two))
    upstream = r.out_grad[...].astype(FULL)
    r.base[...] = (
        upstream
        + scale_two * exact(gap_col * (first_col - second_col), router)
        - resid_f * (scale_two * scale_two * scale_two) * (inner_col / features)
    )

    finish(1)
    weight_grads(cuts // 2, cuts)
    backs_arrive(1)
    moe_grad = fast(r.across[:count, :], backs[1][...])
    moe_grad = moe_grad + fast(r.across[count:, :], backs[1][...])
    resid_grad = r.base[...] + scale_two * moe_grad
    r.resid_grad[...] = resid_grad
    sgrad_launch(exact(c_side, grow_wide * resid_grad))
    finish(0)

    normed = r.normed[...]
    pairing_back = exact(b_side, c_side, TN)
    upper = iota((count, count), 0) <= iota((count, count), 1)
    step_wide = spread_heads(step_col)
    lane8 = iota((8, 128), 1)
    row128 = iota((8, 128), 0)
    rate_parts = jnp.zeros((1, 128), FULL)
    for h in range(heads):
        at = slice(h * count, (h + 1) * count)
        own = jnp.where(lane_head == h, resid_grad, 0.0)
        pull = exact(own, normed, NT) * r.mixing[:, at]
        gap = sum_col[:, h : h + 1] - sum_row[h : h + 1, :]
        found = jnp.sum(jnp.sum(pull * gap, axis=0, keepdims=True), axis=1, keepdims=True)
        rate_parts = jnp.where(lane8[0:1] == h, found, rate_parts)
        r.stack[at, :] = own
    for h in range(heads):
        at = slice(h * count, (h + 1) * count)
        rise = -(run_col[:, h : h + 1] + sum_row[h : h + 1, :] * rate[0:1, h : h + 1])
        table = jnp.where(upper, jnp.exp(jnp.where(upper, rise, 0.0)), 0.0)
        r.mixing[:, at] = table * pairing_back
    local_grad = step_wide * exact(r.mixing[...], r.stack[...]) + skip_wide * resid_grad
    skip_lanes = jnp.sum(resid_grad * normed, axis=0, keepdims=True)
    rate_lanes = jnp.sum(resid_grad * r.carried[...] * sum_wide, axis=0, keepdims=True)
    down_grads(0, down_cuts // 2)

    sgrad_arrive()
    state_grad = carry(r.sgrad_all, True)
    tail_grad = tail_wide * exact(b_side, state_grad, TN)
    normed_grad = local_grad + tail_grad
    last_launch(exact(ones_row, normed_grad * inputs, NT))
    sum_end = sum_wide[count - 1 : count, :]
    rate_lanes = rate_lanes + jnp.sum(
        normed * tail_grad * (sum_end - sum_wide), axis=0, keepdims=True
    )
    rate_lanes = rate_lanes + sum_end * decay_wide * jnp.sum(
        state_grad * state_in, axis=0, keepdims=True
    )
    head_hot = (iota((width, 128), 0) // head_dim == iota((width, 128), 1)).astype(FULL)
    row_wide = iota((8, width), 0)
    lanes = jnp.where(row_wide == 0, rate_lanes, jnp.where(row_wide == 1, skip_lanes, 0.0))
    small_part = exact(lanes, head_hot)
    small_part = jnp.where(row128 == 0, -(small_part + rate_parts), small_part)
    small_launch(small_part)

    down_grads(down_cuts // 2, down_cuts)
    backs_arrive(0)
    first_out = fast(r.across[:count, :], backs[0][...])
    second_out = fast(r.across[count:, :], backs[0][...])
    r.block_out[...] = (resid_f + (weight_one * first_out + weight_two * second_out)).astype(HALF)
    router_arrive()
    router_total = jnp.sum(r.rout_all[...], axis=0)
    r.router_grad[...] = router_total[1 : 1 + experts]

    last_arrive()
    inner_one = to_columns(jnp.sum(r.last_all[...], axis=0))[:, 0:1]
    r.token_grad[...] = (
        resid_grad
        + scale_one * normed_grad
        - inputs * (scale_one * scale_one * scale_one) * (inner_one / features)
    ).astype(HALF)
    small_arrive()
    r.small[...] = jnp.sum(r.small_all[...], axis=0)

    for sent in (
        square_sent,
        decay_sent,
        state_sent,
        stat_sent,
        inner_sent,
        sgrad_sent,
        router_sent,
        last_sent,
        small_sent,
        slot_sent,
        value_sent,
    ):
        sent()
    for t in range(2):

        def sent_back(n):
            back_copy(t, n + 1, block).wait_send()
            z_copy(t, n + 1, block).wait_send()

        loop(blocks - 1, sent_back)
        loop(chip_count, lambda c: pair_copy(t, c).wait_send())
        loop(chip_count - 1, lambda q: chip_copy(t, q + 1).wait_send())

        def spread_done(n):
            k, q = (n // (chip_count - 1), lax.rem(n, chip_count - 1) + 1)
            spread_copy(t, k, origin_of(k), q, place).wait_send()

        loop(blocks * (chip_count - 1), spread_done)

        def partner_done(n):
            k, q = (n // chip_count, lax.rem(n, chip_count))
            partner_copy(t, k, origin_of(k), q, place).wait_send()

        loop(blocks * chip_count, partner_done)


def body(
    tokens,
    routes,
    dt_raw,
    b_proj,
    c_proj,
    decay_rate,
    skip_gain,
    router_weight,
    gate_weight,
    up_weight,
    down_weight,
    out_grad,
):
    peers, blocks = (lax.axis_size(DP), lax.axis_size(EXPERT))
    chip_count = peers // 2
    count, width = tokens.shape
    features, units = gate_weight.shape[1:]
    experts, heads, state = (router_weight.shape[1], decay_rate.shape[0], b_proj.shape[1])
    capacity = 5 * count // (2 * blocks)
    cap = -(-capacity // 16) * 16
    total = blocks * cap
    fused = units % 128 == 0
    stat_rows = -(-(1 + experts) // 8) * 8
    vmem = pl.BlockSpec(memory_space=pltpu.VMEM)
    hbm = pl.BlockSpec(memory_space=pl.ANY)
    dma = pltpu.SemaphoreType.DMA
    given = dict(
        tokens=(tokens, vmem),
        routes=(routes.T, vmem),
        dt=(dt_raw.T, vmem),
        b_proj=(b_proj.T, vmem),
        c_proj=(c_proj.T, vmem),
        rate=(decay_rate[None], vmem),
        skip=(skip_gain[None], vmem),
        router=(router_weight.T, vmem),
        gate_hbm=(gate_weight, hbm),
        up_hbm=(up_weight, hbm),
        down_hbm=(down_weight, hbm),
        out_grad=(out_grad, vmem),
    )
    made = dict(
        block_out=((count, width), HALF),
        token_grad=((count, width), HALF),
        gate_grad=((features, units), HALF),
        up_grad=((features, units), HALF),
        down_grad=((units, features), HALF),
        router_grad=((experts, width), FULL),
        small=((8, 128), FULL),
    )
    if fused:
        split = dict(
            gu_w=((features, 2 * units), HALF),
            gu_s=((total, 2 * units), FULL),
            gu_back=((total, 2 * units), HALF),
            gu_back2=((total, 2 * units), HALF),
        )
    else:
        split = dict(
            gate_w=((features, units), HALF),
            gate_s=((total, units), FULL),
            gate_back=((total, units), HALF),
            gate_back2=((total, units), HALF),
            up_w=((features, units), HALF),
            up_s=((total, units), FULL),
            up_back=((total, units), HALF),
            up_back2=((total, units), HALF),
        )
    scratch = dict(
        split,
        down_w=((units, features), HALF),
        rows=((total, features), HALF),
        grads=((total, features), HALF),
        send_rows=((total, width), HALF),
        send_grads=((total, width), HALF),
        back_f=((total, width), HALF),
        back_b=((total, width), HALF),
        unit_raw=((total, units), FULL),
        hidden=((total, units), HALF),
        hidden2=((total, units), HALF),
        away=((2, chip_count, total, width), HALF),
        mine=((2, chip_count, total, width), HALF),
        pair=((2, chip_count, total, width), HALF),
        chips=((2, chip_count, total, width), HALF),
        summed=((2, total, width), HALF),
        table=((total, 2 * count), FULL),
        across=((2 * count, total), HALF),
        normed=((count, width), FULL),
        local=((count, width), FULL),
        carried=((count, width), FULL),
        base=((count, width), FULL),
        resid_grad=((count, width), FULL),
        resid=((count, width), HALF),
        mixing=((count, heads * count), FULL),
        stack=((heads * count, width), FULL),
        slot_weight=((total, 128), FULL),
        slot_scale=((total, 128), FULL),
        values=((total, 128), FULL),
        slot_src=((blocks, 8, 128), FULL),
        slot_all=((blocks, 8, 128), FULL),
        value_src=((blocks, 8, 128), FULL),
        value_all=((blocks, 8, 128), FULL),
    )
    exchanged = dict(
        square=(DP, (8, count)),
        decay=(EXPERT, (8, width)),
        state=(EXPERT, (state, width)),
        stat=(DP, (stat_rows, count)),
        inner=(DP, (8, 2 * count)),
        sgrad=(EXPERT, (state, width)),
        rout=(EXPERT, (stat_rows, width)),
        last=(DP, (8, count)),
        small=(EXPERT, (8, 128)),
    )
    counts = dict(slot=blocks, value=blocks)
    for name, (axis, shape) in exchanged.items():
        counts[name] = lax.axis_size(axis)
        scratch[name + SRC] = (shape, FULL)
        scratch[name + ALL] = ((counts[name],) + shape, FULL)
    shapes = {name: (amount,) for name, amount in counts.items()}
    shapes.update(
        z=(2, blocks),
        c=(2, blocks * chip_count),
        p=(2, blocks * chip_count),
        pair=(2, chip_count),
        chip=(2, chip_count),
        back=(2, blocks),
    )
    sems = {name + way: dma(shape) for name, shape in shapes.items() for way in (SEND, RECV)}
    sems.update(local_sem=dma((2,)), weight_sem=dma((3,)))
    names = [*given, *made, *scratch, *sems]
    block_out, token_grad, gate_part, up_part, down_part, router_part, small = pl.pallas_call(
        functools.partial(step_kernel, names, capacity, cap, fused),
        out_shape=[jax.ShapeDtypeStruct(shape, kind) for shape, kind in made.values()],
        in_specs=[spec for _, spec in given.values()],
        out_specs=[vmem] * len(made),
        scratch_shapes=[pltpu.VMEM(shape, kind) for shape, kind in scratch.values()]
        + list(sems.values()),
        compiler_params=pltpu.CompilerParams(
            collective_id=7, has_side_effects=True, vmem_limit_bytes=40 << 20
        ),
        name="step",
    )(*[array for array, _ in given.values()])
    return (
        block_out,
        token_grad,
        gate_part[None],
        up_part[None],
        down_part[None],
        router_part.T,
        small[0, :heads],
        small[1, :heads],
    )


def solution(mesh):
    return jax.shard_map(
        body,
        mesh=mesh,
        in_specs=(
            P(EXPERT, DP),
            P(EXPERT, None),
            P(EXPERT, DP),
            P(EXPERT, None),
            P(EXPERT, None),
            P(DP),
            P(DP),
            P(DP, None),
            P(EXPERT, None, DP),
            P(EXPERT, None, DP),
            P(EXPERT, DP, None),
            P(EXPERT, DP),
        ),
        out_specs=(
            P(EXPERT, DP),
            P(EXPERT, DP),
            P(EXPERT, None, DP),
            P(EXPERT, None, DP),
            P(EXPERT, DP, None),
            P(DP, None),
            P(DP),
            P(DP),
        ),
        check_vma=False,
    )
```

```python
import functools
import types
import jax
import jax.numpy as jnp
from jax import lax
from jax.experimental import pallas as pl
from jax.experimental.pallas import tpu as pltpu
from jax.sharding import PartitionSpec as P


EPSILON = 1e-06
HIGHEST = lax.Precision.HIGHEST
MESH = pl.DeviceIdType.MESH
DP, EXPERT = ("dp", "expert")
SEND, RECV, SRC, ALL, SEMS, HBM = ("_send", "_recv", "_src", "_all", "_sems", "_hbm")
HALF, FULL = (jnp.bfloat16, jnp.float32)
NN = (((1,), (0,)), ((), ()))
NT = (((1,), (1,)), ((), ()))
TN = (((0,), (0,)), ((), ()))


def loop(count, step):
    def run(i, carry):
        step(i)
        return carry

    lax.fori_loop(0, count, run, 0)


def slices(total, width):
    return [(at, min(width, total - at)) for at in range(0, total, width)]


def exact(a, b, dims=NN):
    return lax.dot_general(a, b, dims, precision=HIGHEST, preferred_element_type=FULL)


def fast(a, b, dims=NN):
    return lax.dot_general(a, b, dims, preferred_element_type=FULL)


def iota(shape, axis):
    return lax.broadcasted_iota(jnp.int32, shape, axis)


def softplus(v):
    return jnp.maximum(v, 0.0) + jnp.log(1.0 + jnp.exp(-jnp.abs(v)))


def sigmoid(v):
    return 0.5 + 0.5 * jnp.tanh(0.5 * v)


def step_kernel(names, loaded, capacity, cap, fused, *refs):
    r = types.SimpleNamespace(**dict(zip(names, refs)))
    peers, place = (lax.axis_size(DP), lax.axis_index(DP))
    blocks, block = (lax.axis_size(EXPERT), lax.axis_index(EXPERT))
    chip_count = peers // 2
    chip, core = (place // 2, lax.rem(place, 2))
    partner = place + 1 - 2 * core
    count, width = r.tokens.shape
    features = width * peers
    heads = r.dt.shape[0]
    head_dim = width // heads
    experts = r.router.shape[0]
    units = r.down_w.shape[0]
    total = blocks * cap
    stat_rows = r.stat_src.shape[0]
    rows, grads = (r.rows, r.grads)
    sources, wholes = ((r.send_rows, r.send_grads), (rows, grads))
    away, mine, pair, chips = (r.away, r.mine, r.pair, r.chips)
    summed = r.summed
    backs = (r.back_f, r.back_b)
    down_w = r.down_w

    def strip(j):
        return pl.ds(pl.multiple_of(j * cap, 16), cap)

    def columns(d):
        return pl.ds(pl.multiple_of(d * width, 128), width)

    def ahead(k):
        return lax.rem(block + k, blocks)

    def origin_of(k):
        return lax.rem(block + blocks - k, blocks)

    square = chip_count == 4

    def turn(along_u, along_v):
        along_x = (1 - core) * along_u + core * along_v
        along_y = core * along_u + (1 - core) * along_v
        x = lax.rem(lax.rem(chip, 2) + along_x, 2)
        return 2 * lax.rem(chip // 2 + along_y, 2) + x

    def chip_to(way):
        if square:
            return turn((1, 0, 1)[way], (0, 1, 1)[way])
        return lax.rem(chip + way + 1, chip_count)

    def chip_from(way):
        return chip_to(way) if square else lax.rem(chip + chip_count - way - 1, chip_count)

    def partner_chip(way):
        if way < 0:
            return chip
        return chip_to((1, 0, 2)[way]) if square else chip_from(way)

    def chip_in_turn(q):
        if square:
            x = lax.rem(lax.rem(chip, 2) + 1 - q // 2, 2)
            return 2 * lax.rem(chip // 2 + 1 - lax.rem(q, 2), 2) + x
        return lax.rem(chip + q + 1, chip_count)

    if fused:
        gu_w, gu_s = ((r.gu_w,), (r.gu_s,))
        gu_back, gu_back2 = ((r.gu_back,), (r.gu_back2,))
        halves = (r.gu_w.at[:, :units], r.gu_w.at[:, units:])

        def part(group, which, row, at, span):
            lo = at + which * units
            return group[0].at[row, lo : lo + span]
    else:
        gu_w, gu_s = ((r.gate_w, r.up_w), (r.gate_s, r.up_s))
        gu_back = (r.gate_back, r.up_back)
        gu_back2 = (r.gate_back2, r.up_back2)
        halves = (r.gate_w, r.up_w)

        def part(group, which, row, at, span):
            return group[which].at[row, at : at + span]

    weights = [
        pltpu.make_async_copy(hbm.at[0], held, r.weight_sem.at[n])
        for n, (hbm, held) in enumerate(
            ((r.down_hbm, down_w), (r.gate_hbm, halves[0]), (r.up_hbm, halves[1]))
        )
    ]
    loads = {
        name: pltpu.make_async_copy(getattr(r, name + HBM), getattr(r, name), r.load_sem.at[n])
        for n, name in enumerate(loaded)
    }
    for item in loads.values():
        item.start()

    barrier = pltpu.get_barrier_semaphore()
    for axis, amount, me in ((DP, peers, place), (EXPERT, blocks, block)):

        def signal(k):
            pl.semaphore_signal(
                barrier, 1, device_id={axis: lax.rem(me + k + 1, amount)}, device_id_type=MESH
            )

        loop(amount - 1, signal)

    def waits(ref, sems):
        whole = pltpu.make_async_remote_copy(
            src_ref=ref,
            dst_ref=ref,
            send_sem=sems[0],
            recv_sem=sems[1],
            device_id={DP: partner},
            device_id_type=MESH,
        )
        return whole.wait_recv, whole.wait_send

    def exchange(axis, src, everyone, sems):
        amount, me = (peers, place) if axis == DP else (blocks, block)

        def one(k):
            to = lax.rem(me + k + 1, amount)
            pltpu.make_async_remote_copy(
                src_ref=src(to),
                dst_ref=everyone.at[me],
                send_sem=sems.at[0],
                recv_sem=sems.at[1],
                device_id={axis: to},
                device_id_type=MESH,
            ).start()

        arrive, sent = waits(everyone.at[: amount - 1], (sems.at[0], sems.at[1]))
        return lambda: loop(amount - 1, one), arrive, sent

    def shared(axis, name):
        src, everyone = (getattr(r, name + SRC), getattr(r, name + ALL))
        start, arrive, sent = exchange(axis, lambda _: src, everyone, getattr(r, name + SEMS))

        def launch(value):
            src[...] = value
            start()
            everyone[place if axis == DP else block] = value

        return launch, arrive, sent

    square_launch, square_arrive, square_sent = shared(DP, "square")
    decay_launch, decay_arrive, decay_sent = shared(EXPERT, "decay")
    state_launch, state_arrive, state_sent = shared(EXPERT, "state")
    stat_launch, stat_arrive, stat_sent = shared(DP, "stat")
    inner_launch, inner_arrive, inner_sent = shared(DP, "inner")
    sgrad_launch, sgrad_arrive, sgrad_sent = shared(EXPERT, "sgrad")
    router_launch, router_arrive, router_sent = shared(EXPERT, "rout")
    last_launch, last_arrive, last_sent = shared(DP, "last")
    small_launch, small_arrive, small_sent = shared(EXPERT, "small")
    slot_start, slot_arrive, slot_sent = exchange(
        EXPERT, lambda to: r.slot_src.at[to], r.slot_all, r.slot_sems
    )
    value_start, value_arrive, value_sent = exchange(
        EXPERT, lambda to: r.value_src.at[to], r.value_all, r.value_sems
    )

    def own_copy(t):
        return pltpu.make_async_copy(
            sources[t].at[strip(block), :],
            wholes[t].at[strip(block), columns(place)],
            r.local_sem.at[t],
        )

    def z_copy(t, k, land):
        return pltpu.make_async_remote_copy(
            src_ref=sources[t].at[strip(ahead(k)), :],
            dst_ref=wholes[t].at[strip(land), columns(place)],
            send_sem=r.z_send.at[t],
            recv_sem=r.z_recv.at[t, k - 1],
            device_id={EXPERT: ahead(k)},
            device_id_type=MESH,
        )

    def spread_copy(t, k, way, owner, to):
        cut = wholes[t].at[strip(origin_of(k)), columns(owner)]
        return pltpu.make_async_remote_copy(
            src_ref=cut,
            dst_ref=cut,
            send_sem=r.c_send.at[t],
            recv_sem=r.c_recv.at[t, way, k],
            device_id={DP: 2 * to + core},
            device_id_type=MESH,
        )

    def partner_copy(t, way, owner):
        cut = wholes[t].at[:, columns(owner)]
        return pltpu.make_async_remote_copy(
            src_ref=cut,
            dst_ref=cut,
            send_sem=r.p_send.at[t],
            recv_sem=r.p_recv.at[t, way + 1],
            device_id={DP: partner},
            device_id_type=MESH,
        )

    def dispatch(t):
        own_copy(t).start()
        loop(blocks - 1, lambda k: z_copy(t, k + 1, block).start())

    def forward(t, k):
        for way in range(2 if square and t == 0 else chip_count - 1):
            spread_copy(t, k, way, place, chip_to(way)).start()

    def forward_own(t):
        own_copy(t).wait()
        forward(t, 0)

    def pass_on(t):
        def one(n):
            z_copy(t, n + 1, origin_of(n + 1)).wait_recv()
            forward(t, n + 1)

        loop(blocks - 1, one)
        partner_copy(t, -1, place).start()

    def from_chip(t, way):
        owner = 2 * chip_from(way) + core

        def one(k):
            spread_copy(t, k, way, owner, chip_to(way)).wait_recv()
            if square and t == 0 and way == 0:
                spread_copy(t, k, 2, owner, chip_to(1)).start()

        loop(blocks, one)
        partner_copy(t, way, owner).start()

    def from_partner(t, way):
        partner_copy(t, way, 2 * partner_chip(way) + 1 - core).wait_recv()

    def pair_copy(t, c):
        return pltpu.make_async_remote_copy(
            src_ref=away.at[t, c],
            dst_ref=pair.at[t, c],
            send_sem=r.pair_send.at[t],
            recv_sem=r.pair_recv.at[t, c],
            device_id={DP: partner},
            device_id_type=MESH,
        )

    def chip_copy(t, way, c, to):
        return pltpu.make_async_remote_copy(
            src_ref=mine.at[t, c],
            dst_ref=chips.at[t, way],
            send_sem=r.chip_send.at[t],
            recv_sem=r.chip_recv.at[t, way],
            device_id={DP: 2 * to + core},
            device_id_type=MESH,
        )

    def back_copy(t, k, land):
        return pltpu.make_async_remote_copy(
            src_ref=summed.at[t, strip(ahead(k)), :],
            dst_ref=backs[t].at[strip(land), :],
            send_sem=r.back_send.at[t],
            recv_sem=r.back_recv.at[t],
            device_id={EXPERT: ahead(k)},
            device_id_type=MESH,
        )

    def tiles(t, term, between=None):
        def settle(c):
            pair_copy(t, c).wait_recv()
            mine[t, c] = (r.held[...] + pair[t, c].astype(FULL)).astype(HALF)

        def step(q):
            if between is not None:
                pl.when(q == 2)(between)
            value = term(chip_in_turn(q))
            left, right = (value[:, :width], value[:, width:])
            away[t, chip_in_turn(q)] = jnp.where(core == 0, right, left).astype(HALF)
            pair_copy(t, chip_in_turn(q)).start()

            @pl.when(q > 0)
            def _():
                c = chip_in_turn(q - 1)
                settle(c)
                if square:
                    for way, when in ((0, 1), (1, 2 + core)):

                        @pl.when(q == when)
                        def _():
                            chip_copy(t, way, c, chip_to(0)).start()
                else:
                    chip_copy(t, q - 1, c, c).start()

            r.held[...] = jnp.where(core == 0, left, right)

        loop(chip_count, step)
        settle(chip)

    def combine(t):
        if square:
            c = chip_to(1)
            chip_copy(t, 0, c, c).wait_recv()
            mine[t, c] = (mine[t, c].astype(FULL) + chips[t, 0].astype(FULL)).astype(HALF)
            chip_copy(t, 2, c, c).start()

    def finish(t):
        value = mine[t, chip].astype(FULL)
        for way in range(1 if square else 0, chip_count - 1):
            chip_copy(t, way, chip, chip_to(way)).wait_recv()
            value = value + chips[t, way].astype(FULL)
        summed[t] = value.astype(HALF)
        loop(blocks - 1, lambda k: back_copy(t, k + 1, block).start())
        backs[t][strip(block), :] = summed[t, strip(block), :]

    def backs_arrive(t):
        arrive, _ = waits(
            backs[t].at[: (blocks - 1) * cap], (r.back_send.at[t], r.back_recv.at[t])
        )
        arrive()

    for item in loads.values():
        item.wait()
    for item in weights:
        item.start()
    inputs = r.tokens[...].astype(FULL)
    lane_head = iota((1, width), 1) // head_dim

    def spread_heads(cols):
        wide = jnp.zeros((cols.shape[0], width), FULL)
        for h in range(heads):
            wide = jnp.where(lane_head == h, cols[:, h : h + 1], wide)
        return wide

    ones_row = jnp.ones((8, width), FULL)
    square_part = exact(ones_row, inputs * inputs, NT)
    eye8 = (iota((8, 128), 0) == iota((8, 128), 1)).astype(FULL)
    eye_count = (iota((count, count), 0) == iota((count, count), 1)).astype(FULL)

    def to_columns(rows8):
        return exact(rows8, eye8, TN)

    pl.semaphore_wait(barrier, peers + blocks - 2)
    square_launch(square_part)

    routes_row = r.routes[...].astype(FULL)
    routes = exact(eye_count, routes_row, NT)
    expert_row = iota((stat_rows, count), 0).astype(FULL) - 1.0
    first_row = (routes_row[0:1, :] == expert_row).astype(FULL)
    second_row = (routes_row[1:2, :] == expert_row).astype(FULL)
    hot_gap_row = first_row - second_row
    expert_col = iota((count, experts), 1).astype(FULL)
    first_col = (routes[:, 0:1] == expert_col).astype(FULL)
    second_col = (routes[:, 1:2] == expert_col).astype(FULL)
    below = iota((count, count), 0) > iota((count, count), 1)
    above = (iota((count, count), 0) < iota((count, count), 1)).astype(HALF)
    earlier_row = fast((first_row + second_row).astype(HALF), above)
    earlier_col = fast(below.astype(HALF), (first_col + second_col).astype(HALF))

    def slot_of(earlier, hot, ids, axis):
        index = jnp.sum(earlier * hot, axis=axis, keepdims=True)
        return jnp.where(index < capacity, ids * cap + index, -1.0)

    slots_down = iota((total, count), 0).astype(FULL)
    slots_across = iota((count, total), 1).astype(FULL)
    first_table = slots_down == slot_of(earlier_row, first_row, routes_row[0:1, :], 0)
    second_table = slots_down == slot_of(earlier_row, second_row, routes_row[1:2, :], 0)
    first_back = slots_across == slot_of(earlier_col, first_col, routes[:, 0:1], 1)
    second_back = slots_across == slot_of(earlier_col, second_col, routes[:, 1:2], 1)
    either = (first_table | second_table).astype(HALF)
    r.table[:, :count] = first_table.astype(FULL)
    r.table[:, count:] = second_table.astype(FULL)
    r.across[:count, :] = first_back.astype(HALF)
    r.across[count:, :] = second_back.astype(HALF)

    r.send_grads[...] = fast(either, r.out_grad[...]).astype(HALF)
    dispatch(1)

    step_row = softplus(r.dt[...])
    step_col = exact(eye_count, step_row, NT)
    rate = r.rate[...]
    reached = jnp.where(below, 1.0, eye_count)
    sum_col = exact(reached, step_col)
    sum_row = exact(step_row, reached, NT)
    run_col = -sum_col * rate
    decay_end = jnp.exp(run_col[count - 1 : count, :])
    decay_wide = spread_heads(decay_end)
    decay_launch(jnp.broadcast_to(decay_wide, (8, width)))
    tail_col = jnp.exp(run_col[count - 1 : count, :] - run_col) * step_col
    tail_wide = spread_heads(tail_col)
    grow_wide = spread_heads(jnp.exp(run_col))
    skip_wide = spread_heads(r.skip[...])
    sum_wide = spread_heads(sum_col)
    b_side, c_side = (r.b_proj[...], r.c_proj[...])
    forward_own(1)

    square_arrive()
    scale_row_one = lax.rsqrt(jnp.sum(r.square_all[...], axis=0) / features + EPSILON)
    scale_one = to_columns(scale_row_one)[:, 0:1]
    normed = inputs * scale_one
    r.normed[...] = normed
    state_launch(exact(b_side, tail_wide * normed))

    causal = iota((count, count), 0) >= iota((count, count), 1)
    pairing = exact(c_side, b_side, TN)
    for h in range(heads):
        fall = run_col[:, h : h + 1] + sum_row[h : h + 1, :] * rate[0:1, h : h + 1]
        table = jnp.where(causal, jnp.exp(jnp.where(causal, fall, 0.0)), 0.0)
        r.mixing[:, h * count : (h + 1) * count] = table * pairing * step_row[h : h + 1, :]
        r.stack[h * count : (h + 1) * count, :] = jnp.where(lane_head == h, normed, 0.0)
    r.local[...] = exact(r.mixing[...], r.stack[...]) + skip_wide * normed

    pass_on(1)
    decay_arrive()
    state_arrive()

    def carry(states, reverse):
        held = jnp.zeros(r.state_src.shape, FULL)
        for k in range(blocks):
            at = blocks - 1 - k if reverse else k
            reach = at > block if reverse else at < block
            held = jnp.where(reach, r.decay_all[at][0:1, :] * held + states[at], held)
        return held

    state_in = carry(r.state_all, False)
    carried = grow_wide * exact(c_side, state_in, TN)
    r.carried[...] = carried
    resid = (inputs + (r.local[...] + carried)).astype(HALF)
    r.resid[...] = resid
    r.send_rows[...] = fast(either, resid).astype(HALF)
    dispatch(0)
    resid_f = resid.astype(FULL)
    eye_router = (iota((stat_rows, 128), 0) == iota((stat_rows, 128), 1) + 1).astype(FULL)
    router = r.router[...]
    router_row = exact(eye_router[:, :experts], router)
    squares = exact(ones_row[0:1], resid_f * resid_f, NT)
    stat_part = exact(router_row, resid_f, NT)
    stat_launch(jnp.where(iota((stat_rows, count), 0) == 0, squares, stat_part))
    forward_own(0)
    pass_on(0)
    for way in range(chip_count - 1):
        from_chip(1, way)

    stat_arrive()
    stats = jnp.sum(r.stat_all[...], axis=0)
    scale_row = lax.rsqrt(stats[0:1] / features + EPSILON)
    raw_gap = jnp.sum(stats * hot_gap_row, axis=0, keepdims=True)
    first_weight = sigmoid(raw_gap * scale_row)
    second_weight = sigmoid(-raw_gap * scale_row)
    pick8 = iota((8, 2 * count), 0)
    slot_rows = jnp.zeros((8, 2 * count), FULL)
    for n, both in enumerate(((first_weight, second_weight), (scale_row, scale_row))):
        value = jnp.concatenate(both, axis=1)
        near = value.astype(HALF).astype(FULL)
        slot_rows = jnp.where(pick8 == 2 * n, near, slot_rows)
        slot_rows = jnp.where(pick8 == 2 * n + 1, value - near, slot_rows)
    r.slot_src[...] = jnp.zeros_like(r.slot_src)

    slot_wide = fast(slot_rows.astype(HALF), r.table[...].astype(HALF), NT)
    for e in range(blocks):
        r.slot_src[e, :, :cap] = slot_wide[:, e * cap : (e + 1) * cap]
    slot_start()
    r.slot_all[block] = r.slot_src[block]
    weights[1].wait()
    weights[2].wait()
    for held in gu_s:
        held[...] = jnp.zeros_like(held)

    def chunk(d):
        for held, weight in zip(gu_s, gu_w):
            held[...] += fast(rows[:, columns(d)], weight[columns(d), :])

    chunk(place)
    from_chip(0, 0)
    for way in range(-1, chip_count - 1):
        from_partner(1, way)
    weights[0].wait()
    for at, span in slices(units, 256):
        r.unit_raw[:, at : at + span] = fast(grads[...], down_w[at : at + span, :], NT)

    slot_arrive()
    pick = (iota((8, 256), 0) // 2 == iota((8, 256), 1) // 128).astype(HALF)

    wides = [fast(r.slot_all[j].astype(HALF), pick, TN) for j in range(blocks)]
    for j, wide in enumerate(wides):
        r.slot_weight[j * cap : (j + 1) * cap, :] = wide[:cap, :128]
        r.slot_scale[j * cap : (j + 1) * cap, :] = wide[:cap, 128:]

    for way in range(chip_count - 1):
        if way > 0:
            from_chip(0, way)
        from_partner(0, way - 1)

        def one(n):
            other = 2 * partner_chip(way - 1) + 1 - core
            chunk((1 - n) * other + n * (2 * chip_from(way) + core))

        loop(2, one)
    from_partner(0, chip_count - 2)
    chunk(2 * partner_chip(chip_count - 2) + 1 - core)

    tall = 16
    r.values[...] = jnp.zeros_like(r.values)
    span = 128 if units % 128 == 0 else 64

    def some_rows(i):
        row = pl.ds(pl.multiple_of(i * tall, tall), tall)
        scale = r.slot_scale[row, :span]
        weight = r.slot_weight[row, :span]
        first = jnp.zeros((tall, span), FULL)
        second = jnp.zeros((tall, span), FULL)
        spans = range(0, units, span)
        given = [
            (
                part(gu_s, 0, row, at, span)[...],
                part(gu_s, 1, row, at, span)[...],
                r.unit_raw[row, at : at + span],
            )
            for at in spans
        ]
        found = []
        for gate_raw, up_raw, unit_raw in given:
            gate, up = (gate_raw * scale, up_raw * scale)
            sigma = sigmoid(gate)
            silu = gate * sigma
            hid = silu * up
            unit = unit_raw * weight
            gate_b = unit * up * (sigma + silu * (1.0 - sigma))
            up_b = unit * silu
            first = first + hid * unit_raw
            second = second + (gate_b * gate_raw + up_b * up_raw)
            values = (hid, hid * weight, gate_b, up_b, gate_b * scale, up_b * scale)
            found.append([value.astype(HALF) for value in values])
        for at, (hid, hid2, gate_b, up_b, gate_b2, up_b2) in zip(spans, found):
            r.hidden[row, at : at + span] = hid
            r.hidden2[row, at : at + span] = hid2
            part(gu_back, 0, row, at, span)[...] = gate_b
            part(gu_back, 1, row, at, span)[...] = up_b
            part(gu_back2, 0, row, at, span)[...] = gate_b2
            part(gu_back2, 1, row, at, span)[...] = up_b2
        r.values[row, :span] = first
        r.values[row, 128 : 128 + span] = second

    loop(total // tall, some_rows)
    def send_values():
        r.value_src[...] = jnp.zeros_like(r.value_src)
        lane_sums = (iota((8, 256), 0) == iota((8, 256), 1) // 128).astype(FULL)
        value_rows = exact(lane_sums, r.values[...], NT)
        for j in range(blocks):
            r.value_src[j, :, :cap] = value_rows[:, j * cap : (j + 1) * cap]
        value_start()
        r.value_all[block] = r.value_src[block]

    def both_columns(c):
        return pl.ds(pl.multiple_of(2 * c * width, 256), 2 * width)

    def input_term(c):
        result = None
        for back, weight in zip(gu_back, gu_w):
            term = fast(back[...], weight[both_columns(c), :], NT)
            result = term if result is None else result + term
        return result

    def output_term(c):
        return fast(r.hidden[...], down_w[:, both_columns(c)])

    tiles(1, input_term, send_values)

    combine(1)
    value_arrive()
    inner_part = jnp.zeros((8, 2 * count), FULL)
    for j in range(blocks):
        inner_part = inner_part + exact(
            r.value_all[j, :, :cap], r.table[j * cap : (j + 1) * cap, :]
        )
    inner_launch(inner_part)

    tiles(0, output_term)

    wide_cut = 256

    def weight_grads(lo, hi):
        def one(i):
            at = pl.ds(pl.multiple_of(i * wide_cut, wide_cut), wide_cut)
            if fused:
                value = fast(rows[:, at], gu_back2[0][...], TN)
                r.gate_grad[at, :] = value[:, :units].astype(HALF)
                r.up_grad[at, :] = value[:, units:].astype(HALF)
            else:
                r.gate_grad[at, :] = fast(rows[:, at], gu_back2[0][...], TN).astype(HALF)
                r.up_grad[at, :] = fast(rows[:, at], gu_back2[1][...], TN).astype(HALF)

        lax.fori_loop(lo, hi, lambda i, c: (one(i), c)[1], 0)

    cuts = features // wide_cut

    finish(1)
    weight_grads(0, cuts // 2)
    combine(0)
    inner_arrive()
    inner_all = jnp.sum(r.inner_all[...], axis=0)
    gap_grad = first_weight * second_weight * (inner_all[0:1, :count] - inner_all[0:1, count:])
    inner_row = inner_all[1:2, :count] + inner_all[1:2, count:] + gap_grad * raw_gap
    row8 = iota((8, count), 0)
    packed = jnp.where(row8 == 0, scale_row, 0.0)
    packed = jnp.where(row8 == 1, inner_row, packed)
    packed = jnp.where(row8 == 2, gap_grad, packed)
    packed = jnp.where(row8 == 3, first_weight, packed)
    packed = jnp.where(row8 == 4, second_weight, packed)
    packed_cols = to_columns(packed)
    scale_two, inner_col = (packed_cols[:, 0:1], packed_cols[:, 1:2])
    gap_col = packed_cols[:, 2:3]
    weight_one, weight_two = (packed_cols[:, 3:4], packed_cols[:, 4:5])
    resid_f = r.resid[...].astype(FULL)
    router_launch(exact(gap_grad * hot_gap_row, resid_f * scale_two))
    upstream = r.out_grad[...].astype(FULL)
    r.base[...] = (
        upstream
        + scale_two * exact(gap_col * (first_col - second_col), router)
        - resid_f * (scale_two * scale_two * scale_two) * (inner_col / features)
    )

    backs_arrive(1)
    moe_grad = fast(r.across[:count, :], backs[1][...])
    moe_grad = moe_grad + fast(r.across[count:, :], backs[1][...])
    resid_grad = r.base[...] + scale_two * moe_grad
    r.resid_grad[...] = resid_grad
    sgrad_launch(exact(c_side, grow_wide * resid_grad))
    normed = r.normed[...]
    pairing_back = exact(b_side, c_side, TN)
    upper = iota((count, count), 0) <= iota((count, count), 1)
    step_wide = spread_heads(step_col)
    lane8 = iota((8, 128), 1)
    row128 = iota((8, 128), 0)
    rate_parts = jnp.zeros((1, 128), FULL)
    for h in range(heads):
        at = slice(h * count, (h + 1) * count)
        own = jnp.where(lane_head == h, resid_grad, 0.0)
        pull = exact(own, normed, NT) * r.mixing[:, at]
        gap = sum_col[:, h : h + 1] - sum_row[h : h + 1, :]
        found = jnp.sum(jnp.sum(pull * gap, axis=0, keepdims=True), axis=1, keepdims=True)
        rate_parts = jnp.where(lane8[0:1] == h, found, rate_parts)
        r.stack[at, :] = own
    for h in range(heads):
        at = slice(h * count, (h + 1) * count)
        rise = -(run_col[:, h : h + 1] + sum_row[h : h + 1, :] * rate[0:1, h : h + 1])
        table = jnp.where(upper, jnp.exp(jnp.where(upper, rise, 0.0)), 0.0)
        r.mixing[:, at] = table * pairing_back
    local_grad = step_wide * exact(r.mixing[...], r.stack[...]) + skip_wide * resid_grad
    skip_lanes = jnp.sum(resid_grad * normed, axis=0, keepdims=True)
    rate_lanes = jnp.sum(resid_grad * r.carried[...] * sum_wide, axis=0, keepdims=True)
    weight_grads(cuts // 2, 5 * cuts // 8)
    finish(0)
    weight_grads(5 * cuts // 8, cuts)


    sgrad_arrive()
    state_grad = carry(r.sgrad_all, True)
    tail_grad = tail_wide * exact(b_side, state_grad, TN)
    normed_grad = local_grad + tail_grad
    last_launch(exact(ones_row, normed_grad * inputs, NT))
    sum_end = sum_wide[count - 1 : count, :]
    rate_lanes = rate_lanes + jnp.sum(
        normed * tail_grad * (sum_end - sum_wide), axis=0, keepdims=True
    )
    rate_lanes = rate_lanes + sum_end * decay_wide * jnp.sum(
        state_grad * state_in, axis=0, keepdims=True
    )
    head_hot = (iota((width, 128), 0) // head_dim == iota((width, 128), 1)).astype(FULL)
    row_wide = iota((8, width), 0)
    lanes = jnp.where(row_wide == 0, rate_lanes, jnp.where(row_wide == 1, skip_lanes, 0.0))
    small_part = exact(lanes, head_hot)
    small_part = jnp.where(row128 == 0, -(small_part + rate_parts), small_part)
    small_launch(small_part)

    backs_arrive(0)
    first_out = fast(r.across[:count, :], backs[0][...])
    second_out = fast(r.across[count:, :], backs[0][...])
    r.block_out[...] = (resid_f + (weight_one * first_out + weight_two * second_out)).astype(HALF)
    router_arrive()
    router_total = jnp.sum(r.rout_all[...], axis=0)
    r.router_grad[...] = router_total[1 : 1 + experts]

    last_arrive()
    inner_one = to_columns(jnp.sum(r.last_all[...], axis=0))[:, 0:1]
    r.token_grad[...] = (
        resid_grad
        + scale_one * normed_grad
        - inputs * (scale_one * scale_one * scale_one) * (inner_one / features)
    ).astype(HALF)
    small_arrive()
    small = jnp.sum(r.small_all[...], axis=0)
    r.rate_grad[...] = small[0:1, :heads]
    r.skip_grad[...] = small[1:2, :heads]

    for sent in (
        square_sent,
        decay_sent,
        state_sent,
        stat_sent,
        inner_sent,
        sgrad_sent,
        router_sent,
        last_sent,
        small_sent,
        slot_sent,
        value_sent,
    ):
        sent()
    lead = (blocks - 1) * cap
    for t in range(2):
        for ref, send, recv in (
            (sources[t].at[:lead], r.z_send, r.z_recv.at[t, 0]),
            (wholes[t].at[:, : (chip_count - 1) * width], r.c_send, r.c_recv.at[t, 0, 0]),
            (wholes[t].at[:, : chip_count * width], r.p_send, r.p_recv.at[t, 0]),
            (away.at[t], r.pair_send, r.pair_recv.at[t, 0]),
            (mine.at[t, 1:], r.chip_send, r.chip_recv.at[t, 0]),
            (summed.at[t, :lead], r.back_send, r.back_recv.at[t]),
        ):
            waits(ref, (send.at[t], recv))[1]()


PIECES = 4


def write_kernel(hidden, grads, *refs):
    amount = (len(refs) - 2) // 2
    ready, outs, down, sems = (refs[:amount], refs[amount:-2], refs[-2], refs[-1])
    copies = []

    def send(src, dst, rows, at):
        cut = pl.ds(at, rows)
        copies.append(pltpu.make_async_copy(src.at[cut], dst.at[cut], sems.at[len(copies)]))
        copies[-1].start()

    for src, dst in zip(ready, outs):
        rows = src.shape[0]
        pieces = PIECES if rows % (16 * PIECES) == 0 and rows >= 512 else 1
        for at in range(0, rows, rows // pieces):
            send(src, dst, rows // pieces, at)
    for at, rows in slices(down.shape[0], 256):
        down[at : at + rows, :] = fast(hidden[:, at : at + rows], grads[...], TN).astype(HALF)
        send(down, outs[-1], rows, at)
    for copy in copies:
        copy.wait()


def body(
    tokens,
    routes,
    dt_raw,
    b_proj,
    c_proj,
    decay_rate,
    skip_gain,
    router_weight,
    gate_weight,
    up_weight,
    down_weight,
    out_grad,
):
    peers, blocks = (lax.axis_size(DP), lax.axis_size(EXPERT))
    chip_count = peers // 2
    count, width = tokens.shape
    features, units = gate_weight.shape[1:]
    experts, heads, state = (router_weight.shape[1], decay_rate.shape[0], b_proj.shape[1])
    capacity = 5 * count // (2 * blocks)
    cap = -(-capacity // 16) * 16
    total = blocks * cap
    fused = units % 128 == 0
    stat_rows = -(-(1 + experts) // 8) * 8
    vmem = pl.BlockSpec(memory_space=pltpu.VMEM)
    hbm = pl.BlockSpec(memory_space=pltpu.HBM)
    dma = pltpu.SemaphoreType.DMA
    loaded = dict(
        tokens=tokens,
        routes=routes.T,
        dt=dt_raw.T,
        b_proj=b_proj.T,
        c_proj=c_proj.T,
        rate=decay_rate[None],
        skip=skip_gain[None],
        router=router_weight.T,
        out_grad=out_grad,
    )
    given = {name + HBM: array for name, array in loaded.items()}
    given.update(gate_hbm=gate_weight, up_hbm=up_weight, down_hbm=down_weight)
    made = dict(
        block_out=((count, width), HALF),
        token_grad=((count, width), HALF),
        gate_grad=((features, units), HALF),
        up_grad=((features, units), HALF),
        router_grad=((experts, width), FULL),
        rate_grad=((1, heads), FULL),
        skip_grad=((1, heads), FULL),
        hidden2=((total, units), HALF),
        grads=((total, features), HALF),
    )
    if fused:
        split = dict(
            gu_w=((features, 2 * units), HALF),
            gu_s=((total, 2 * units), FULL),
            gu_back=((total, 2 * units), HALF),
            gu_back2=((total, 2 * units), HALF),
        )
    else:
        split = dict(
            gate_w=((features, units), HALF),
            gate_s=((total, units), FULL),
            gate_back=((total, units), HALF),
            gate_back2=((total, units), HALF),
            up_w=((features, units), HALF),
            up_s=((total, units), FULL),
            up_back=((total, units), HALF),
            up_back2=((total, units), HALF),
        )
    scratch = dict(
        split,
        down_w=((units, features), HALF),
        rows=((total, features), HALF),
        send_rows=((total, width), HALF),
        send_grads=((total, width), HALF),
        back_f=((total, width), HALF),
        back_b=((total, width), HALF),
        unit_raw=((total, units), FULL),
        hidden=((total, units), HALF),
        away=((2, chip_count, total, width), HALF),
        mine=((2, chip_count, total, width), HALF),
        pair=((2, chip_count, total, width), HALF),
        chips=((2, chip_count - 1, total, width), HALF),
        summed=((2, total, width), HALF),
        held=((total, width), FULL),
        table=((total, 2 * count), FULL),
        across=((2 * count, total), HALF),
        normed=((count, width), FULL),
        local=((count, width), FULL),
        carried=((count, width), FULL),
        base=((count, width), FULL),
        resid_grad=((count, width), FULL),
        resid=((count, width), HALF),
        mixing=((count, heads * count), FULL),
        stack=((heads * count, width), FULL),
        slot_weight=((total, 128), FULL),
        slot_scale=((total, 128), FULL),
        values=((total, 256), FULL),
        slot_src=((blocks, 8, 128), FULL),
        slot_all=((blocks, 8, 128), FULL),
        value_src=((blocks, 8, 128), FULL),
        value_all=((blocks, 8, 128), FULL),
    )
    exchanged = dict(
        square=(DP, (8, count)),
        decay=(EXPERT, (8, width)),
        state=(EXPERT, (state, width)),
        stat=(DP, (stat_rows, count)),
        inner=(DP, (8, 2 * count)),
        sgrad=(EXPERT, (state, width)),
        rout=(EXPERT, (stat_rows, width)),
        last=(DP, (8, count)),
        small=(EXPERT, (8, 128)),
    )
    sems = dict(slot_sems=dma((2,)), value_sems=dma((2,)))
    for name, (axis, shape) in exchanged.items():
        scratch[name + SRC] = (shape, FULL)
        scratch[name + ALL] = ((lax.axis_size(axis),) + shape, FULL)
        sems[name + SEMS] = dma((2,))
    for name, array in loaded.items():
        scratch[name] = (array.shape, array.dtype)
    shapes = dict(
        z=(2, blocks - 1),
        c=(2, chip_count - 1, blocks),
        p=(2, chip_count),
        pair=(2, chip_count),
        chip=(2, chip_count - 1),
        back=(2,),
    )
    for name, shape in shapes.items():
        sems[name + SEND] = dma((2,))
        sems[name + RECV] = dma(shape)
    sems.update(local_sem=dma((2,)), weight_sem=dma((3,)), load_sem=dma((len(loaded),)))
    names = [*given, *made, *scratch, *sems]
    results = pl.pallas_call(
        functools.partial(step_kernel, names, list(loaded), capacity, cap, fused),
        out_shape=[jax.ShapeDtypeStruct(shape, kind) for shape, kind in made.values()],
        in_specs=[hbm] * len(given),
        out_specs=[vmem] * len(made),
        scratch_shapes=[pltpu.VMEM(shape, kind) for shape, kind in scratch.values()]
        + list(sems.values()),
        compiler_params=pltpu.CompilerParams(
            collective_id=7, has_side_effects=True, vmem_limit_bytes=40 << 20
        ),
        name="step",
    )(*[pltpu.with_memory_space_constraint(x, pltpu.HBM) for x in given.values()])
    *ready, hidden, grads = results
    shapes = [*ready, jax.ShapeDtypeStruct((units, features), HALF)]
    block_out, token_grad, gate_part, up_part, router_part, rate, skip, down_part = pl.pallas_call(
        write_kernel,
        out_shape=[jax.ShapeDtypeStruct(like.shape, like.dtype) for like in shapes],
        in_specs=[vmem] * len(results),
        out_specs=[hbm] * len(shapes),
        scratch_shapes=[pltpu.VMEM((units, features), HALF), dma((len(shapes) * PIECES,))],
        compiler_params=pltpu.CompilerParams(vmem_limit_bytes=12 << 20),
        name="write",
    )(hidden, grads, *ready)
    return (
        block_out,
        token_grad,
        gate_part[None],
        up_part[None],
        down_part[None],
        router_part.T,
        rate[0],
        skip[0],
    )


def solution(mesh):
    return jax.shard_map(
        body,
        mesh=mesh,
        in_specs=(
            P(EXPERT, DP),
            P(EXPERT, None),
            P(EXPERT, DP),
            P(EXPERT, None),
            P(EXPERT, None),
            P(DP),
            P(DP),
            P(DP, None),
            P(EXPERT, None, DP),
            P(EXPERT, None, DP),
            P(EXPERT, DP, None),
            P(EXPERT, DP),
        ),
        out_specs=(
            P(EXPERT, DP),
            P(EXPERT, DP),
            P(EXPERT, None, DP),
            P(EXPERT, None, DP),
            P(EXPERT, DP, None),
            P(DP, None),
            P(DP),
            P(DP),
        ),
        check_vma=False,
    )
```

```python
import functools
import types
import jax
import jax.numpy as jnp
from jax import lax
from jax.experimental import pallas as pl
from jax.experimental.pallas import tpu as pltpu
from jax.sharding import PartitionSpec as P


EPSILON = 1e-06
HIGHEST = lax.Precision.HIGHEST
MESH = pl.DeviceIdType.MESH
DP, EXPERT = ("dp", "expert")
SEND, RECV, SRC, ALL, SEMS, HBM = ("_send", "_recv", "_src", "_all", "_sems", "_hbm")
HALF, FULL = (jnp.bfloat16, jnp.float32)
NN = (((1,), (0,)), ((), ()))
NT = (((1,), (1,)), ((), ()))
TN = (((0,), (0,)), ((), ()))


def loop(count, step):
    def run(i, carry):
        step(i)
        return carry

    lax.fori_loop(0, count, run, 0)


def slices(total, width):
    return [(at, min(width, total - at)) for at in range(0, total, width)]


def exact(a, b, dims=NN):
    return lax.dot_general(a, b, dims, precision=HIGHEST, preferred_element_type=FULL)


def fast(a, b, dims=NN):
    return lax.dot_general(a, b, dims, preferred_element_type=FULL)


def iota(shape, axis):
    return lax.broadcasted_iota(jnp.int32, shape, axis)


def softplus(v):
    return jnp.maximum(v, 0.0) + jnp.log(1.0 + jnp.exp(-jnp.abs(v)))


def sigmoid(v):
    return 0.5 + 0.5 * jnp.tanh(0.5 * v)


def step_kernel(names, loaded, capacity, cap, fused, *refs):
    r = types.SimpleNamespace(**dict(zip(names, refs)))
    peers, place = (lax.axis_size(DP), lax.axis_index(DP))
    blocks, block = (lax.axis_size(EXPERT), lax.axis_index(EXPERT))
    chip_count = peers // 2
    chip, core = (place // 2, lax.rem(place, 2))
    partner = place + 1 - 2 * core
    count, width = r.tokens.shape
    features = width * peers
    heads = r.dt.shape[0]
    head_dim = width // heads
    experts = r.router.shape[0]
    units = r.down_w.shape[0]
    total = blocks * cap
    stat_rows = r.stat_src.shape[0]
    rows, grads = (r.rows, r.grads)
    sources, wholes = ((r.send_rows, r.send_grads), (rows, grads))
    away, mine, pair, chips = (r.away, r.mine, r.pair, r.chips)
    summed = r.summed
    backs = (r.back_f, r.back_b)
    down_w = r.down_w

    def strip(j):
        return pl.ds(pl.multiple_of(j * cap, 16), cap)

    def columns(d):
        return pl.ds(pl.multiple_of(d * width, 128), width)

    def ahead(k):
        return lax.rem(block + k, blocks)

    def origin_of(k):
        return lax.rem(block + blocks - k, blocks)

    square = chip_count == 4

    def turn(along_u, along_v):
        along_x = (1 - core) * along_u + core * along_v
        along_y = core * along_u + (1 - core) * along_v
        x = lax.rem(lax.rem(chip, 2) + along_x, 2)
        return 2 * lax.rem(chip // 2 + along_y, 2) + x

    def chip_to(way):
        if square:
            return turn((1, 0, 1)[way], (0, 1, 1)[way])
        return lax.rem(chip + way + 1, chip_count)

    def chip_from(way):
        return chip_to(way) if square else lax.rem(chip + chip_count - way - 1, chip_count)

    def partner_chip(way):
        if way < 0:
            return chip
        return chip_to((1, 0, 2)[way]) if square else chip_from(way)

    def chip_in_turn(q):
        if square:
            x = lax.rem(lax.rem(chip, 2) + 1 - q // 2, 2)
            return 2 * lax.rem(chip // 2 + 1 - lax.rem(q, 2), 2) + x
        return lax.rem(chip + q + 1, chip_count)

    if fused:
        gu_w, gu_s = ((r.gu_w,), (r.gu_s,))
        gu_back, gu_back2 = ((r.gu_back,), (r.gu_back2,))
        halves = (r.gu_w.at[:, :units], r.gu_w.at[:, units:])

        def part(group, which, row, at, span):
            lo = at + which * units
            return group[0].at[row, lo : lo + span]
    else:
        gu_w, gu_s = ((r.gate_w, r.up_w), (r.gate_s, r.up_s))
        gu_back = (r.gate_back, r.up_back)
        gu_back2 = (r.gate_back2, r.up_back2)
        halves = (r.gate_w, r.up_w)

        def part(group, which, row, at, span):
            return group[which].at[row, at : at + span]

    weights = [
        pltpu.make_async_copy(hbm.at[0], held, r.weight_sem.at[n])
        for n, (hbm, held) in enumerate(
            ((r.down_hbm, down_w), (r.gate_hbm, halves[0]), (r.up_hbm, halves[1]))
        )
    ]
    loads = {
        name: pltpu.make_async_copy(getattr(r, name + HBM), getattr(r, name), r.load_sem.at[n])
        for n, name in enumerate(loaded)
    }
    for item in loads.values():
        item.start()

    barrier = pltpu.get_barrier_semaphore()
    for axis, amount, me in ((DP, peers, place), (EXPERT, blocks, block)):

        def signal(k):
            pl.semaphore_signal(
                barrier, 1, device_id={axis: lax.rem(me + k + 1, amount)}, device_id_type=MESH
            )

        loop(amount - 1, signal)

    def waits(ref, sems):
        whole = pltpu.make_async_remote_copy(
            src_ref=ref,
            dst_ref=ref,
            send_sem=sems[0],
            recv_sem=sems[1],
            device_id={DP: partner},
            device_id_type=MESH,
        )
        return whole.wait_recv, whole.wait_send

    def exchange(axis, src, everyone, sems):
        amount, me = (peers, place) if axis == DP else (blocks, block)

        def one(k):
            to = lax.rem(me + k + 1, amount)
            pltpu.make_async_remote_copy(
                src_ref=src(to),
                dst_ref=everyone.at[me],
                send_sem=sems.at[0],
                recv_sem=sems.at[1],
                device_id={axis: to},
                device_id_type=MESH,
            ).start()

        arrive, sent = waits(everyone.at[: amount - 1], (sems.at[0], sems.at[1]))
        return lambda: loop(amount - 1, one), arrive, sent

    def shared(axis, name):
        src, everyone = (getattr(r, name + SRC), getattr(r, name + ALL))
        start, arrive, sent = exchange(axis, lambda _: src, everyone, getattr(r, name + SEMS))

        def launch(value):
            value = value.astype(src.dtype)
            src[...] = value
            start()
            everyone[place if axis == DP else block] = value

        return launch, arrive, sent

    square_launch, square_arrive, square_sent = shared(DP, "square")
    decay_launch, decay_arrive, decay_sent = shared(EXPERT, "decay")
    state_launch, state_arrive, state_sent = shared(EXPERT, "state")
    stat_launch, stat_arrive, stat_sent = shared(DP, "stat")
    inner_launch, inner_arrive, inner_sent = shared(DP, "inner")
    sgrad_launch, sgrad_arrive, sgrad_sent = shared(EXPERT, "sgrad")
    router_launch, router_arrive, router_sent = shared(EXPERT, "rout")
    last_launch, last_arrive, last_sent = shared(DP, "last")
    small_launch, small_arrive, small_sent = shared(EXPERT, "small")
    slot_start, slot_arrive, slot_sent = exchange(
        EXPERT, lambda to: r.slot_src.at[to], r.slot_all, r.slot_sems
    )
    value_start, value_arrive, value_sent = exchange(
        EXPERT, lambda to: r.value_src.at[to], r.value_all, r.value_sems
    )

    def own_copy(t):
        return pltpu.make_async_copy(
            sources[t].at[strip(block), :],
            wholes[t].at[strip(block), columns(place)],
            r.local_sem.at[t],
        )

    def z_copy(t, k, land):
        return pltpu.make_async_remote_copy(
            src_ref=sources[t].at[strip(ahead(k)), :],
            dst_ref=wholes[t].at[strip(land), columns(place)],
            send_sem=r.z_send.at[t],
            recv_sem=r.z_recv.at[t, k - 1],
            device_id={EXPERT: ahead(k)},
            device_id_type=MESH,
        )

    def spread_copy(t, k, way, owner, to):
        cut = wholes[t].at[strip(origin_of(k)), columns(owner)]
        return pltpu.make_async_remote_copy(
            src_ref=cut,
            dst_ref=cut,
            send_sem=r.c_send.at[t],
            recv_sem=r.u_recv.at[k] if (t, way) == (0, 0) else r.c_recv.at[t, way],
            device_id={DP: 2 * to + core},
            device_id_type=MESH,
        )

    def partner_copy(t, way, owner):
        cut = wholes[t].at[:, columns(owner)]
        return pltpu.make_async_remote_copy(
            src_ref=cut,
            dst_ref=cut,
            send_sem=r.p_send.at[t],
            recv_sem=r.p_recv.at[t, way + 1],
            device_id={DP: partner},
            device_id_type=MESH,
        )

    def dispatch(t):
        own_copy(t).start()
        loop(blocks - 1, lambda k: z_copy(t, k + 1, block).start())

    def forward(t, k):
        for way in range(2 if square and t == 0 else chip_count - 1):
            spread_copy(t, k, way, place, chip_to(way)).start()

    def forward_own(t):
        own_copy(t).wait()
        forward(t, 0)

    def pass_on(t):
        def one(n):
            z_copy(t, n + 1, origin_of(n + 1)).wait_recv()
            forward(t, n + 1)

        loop(blocks - 1, one)
        partner_copy(t, -1, place).start()

    def from_chip(t, way):
        owner = 2 * chip_from(way) + core
        cut = wholes[t].at[:, columns(owner)]
        waits(cut, (r.c_send.at[t], r.c_recv.at[t, way]))[0]()
        partner_copy(t, way, owner).start()

    def relay(k):
        owner = 2 * chip_from(0) + core
        spread_copy(0, k, 0, owner, chip_to(0)).wait_recv()
        if square:
            spread_copy(0, k, 2, owner, chip_to(1)).start()
        if k == blocks - 1:
            partner_copy(0, 0, owner).start()

    def from_partner(t, way):
        partner_copy(t, way, 2 * partner_chip(way) + 1 - core).wait_recv()

    def pair_copy(t, c):
        return pltpu.make_async_remote_copy(
            src_ref=away.at[t, c],
            dst_ref=pair.at[t, c],
            send_sem=r.pair_send.at[t],
            recv_sem=r.pair_recv.at[t, c],
            device_id={DP: partner},
            device_id_type=MESH,
        )

    def chip_copy(t, way, c, to):
        return pltpu.make_async_remote_copy(
            src_ref=mine.at[t, c],
            dst_ref=chips.at[t, way],
            send_sem=r.chip_send.at[t],
            recv_sem=r.chip_recv.at[t, way],
            device_id={DP: 2 * to + core},
            device_id_type=MESH,
        )

    def piece_copy(t, way, n, c, to):
        return pltpu.make_async_remote_copy(
            src_ref=mine.at[t, c, strip(ahead(n + 1))],
            dst_ref=chips.at[t, way, strip(ahead(n + 1))],
            send_sem=r.chip_send.at[t],
            recv_sem=r.piece_recv.at[t, way // 2, n],
            device_id={DP: 2 * to + core},
            device_id_type=MESH,
        )

    def back_copy(t, k, land):
        return pltpu.make_async_remote_copy(
            src_ref=summed.at[t, strip(ahead(k)), :],
            dst_ref=backs[t].at[strip(land), :],
            send_sem=r.back_send.at[t],
            recv_sem=r.back_recv.at[t],
            device_id={EXPERT: ahead(k)},
            device_id_type=MESH,
        )

    def tiles(t, term, when, between):
        def settle(c):
            pair_copy(t, c).wait_recv()
            mine[t, c] = (r.held[...] + pair[t, c].astype(FULL)).astype(HALF)

        def step(q):
            pl.when(q == when)(between)
            value = term(chip_in_turn(q))
            left, right = (value[:, :width], value[:, width:])
            away[t, chip_in_turn(q)] = jnp.where(core == 0, right, left).astype(HALF)
            pair_copy(t, chip_in_turn(q)).start()

            @pl.when(q > 0)
            def _():
                c = chip_in_turn(q - 1)
                settle(c)
                if square:

                    @pl.when(q == 1)
                    def _():
                        loop(blocks, lambda n: piece_copy(t, 0, n, c, chip_to(0)).start())

                    @pl.when(q == 2 + core)
                    def _():
                        chip_copy(t, 1, c, chip_to(0)).start()
                else:
                    chip_copy(t, q - 1, c, c).start()

            r.held[...] = jnp.where(core == 0, left, right)

        loop(chip_count, step)
        settle(chip)

    def combine(t):
        if square:
            c = chip_to(1)

            def one(n):
                piece_copy(t, 0, n, c, c).wait_recv()
                row = strip(ahead(n + 1))
                value = mine[t, c, row].astype(FULL) + chips[t, 0, row].astype(FULL)
                mine[t, c, row] = value.astype(HALF)
                piece_copy(t, 2, n, c, c).start()

            loop(blocks, one)

    def finish(t):
        wholes_in = (1,) if square else range(chip_count - 1)
        for way in wholes_in:
            chip_copy(t, way, chip, chip_to(way)).wait_recv()

        def one(n):
            row = strip(ahead(n + 1))
            value = mine[t, chip, row].astype(FULL)
            if square:
                piece_copy(t, 2, n, chip, chip).wait_recv()
            for way in range(1 if square else 0, chip_count - 1):
                value = value + chips[t, way, row].astype(FULL)
            summed[t, row] = value.astype(HALF)

            @pl.when(n < blocks - 1)
            def _():
                back_copy(t, n + 1, block).start()

        loop(blocks, one)
        backs[t][strip(block), :] = summed[t, strip(block), :]

    def backs_arrive(t):
        arrive, _ = waits(
            backs[t].at[: (blocks - 1) * cap], (r.back_send.at[t], r.back_recv.at[t])
        )
        arrive()

    for item in loads.values():
        item.wait()
    for item in weights:
        item.start()
    inputs = r.tokens[...].astype(FULL)
    lane_head = iota((1, width), 1) // head_dim

    def spread_heads(cols):
        wide = jnp.zeros((cols.shape[0], width), FULL)
        for h in range(heads):
            wide = jnp.where(lane_head == h, cols[:, h : h + 1], wide)
        return wide

    ones_row = jnp.ones((8, width), FULL)
    square_part = exact(ones_row, inputs * inputs, NT)
    eye8 = (iota((8, 128), 0) == iota((8, 128), 1)).astype(FULL)
    eye_count = (iota((count, count), 0) == iota((count, count), 1)).astype(FULL)

    def to_columns(rows8):
        return exact(rows8, eye8, TN)

    pl.semaphore_wait(barrier, peers + blocks - 2)
    square_launch(square_part)

    routes_row = r.routes[...].astype(FULL)
    routes = exact(eye_count, routes_row, NT)
    expert_row = iota((stat_rows, count), 0).astype(FULL) - 1.0
    first_row = (routes_row[0:1, :] == expert_row).astype(FULL)
    second_row = (routes_row[1:2, :] == expert_row).astype(FULL)
    hot_gap_row = first_row - second_row
    expert_col = iota((count, experts), 1).astype(FULL)
    first_col = (routes[:, 0:1] == expert_col).astype(FULL)
    second_col = (routes[:, 1:2] == expert_col).astype(FULL)
    below = iota((count, count), 0) > iota((count, count), 1)
    above = (iota((count, count), 0) < iota((count, count), 1)).astype(HALF)
    earlier_row = fast((first_row + second_row).astype(HALF), above)
    earlier_col = fast(below.astype(HALF), (first_col + second_col).astype(HALF))

    def slot_of(earlier, hot, ids, axis):
        index = jnp.sum(earlier * hot, axis=axis, keepdims=True)
        return jnp.where(index < capacity, ids * cap + index, -1.0)

    slots_down = iota((total, count), 0).astype(FULL)
    slots_across = iota((count, total), 1).astype(FULL)
    first_table = slots_down == slot_of(earlier_row, first_row, routes_row[0:1, :], 0)
    second_table = slots_down == slot_of(earlier_row, second_row, routes_row[1:2, :], 0)
    first_back = slots_across == slot_of(earlier_col, first_col, routes[:, 0:1], 1)
    second_back = slots_across == slot_of(earlier_col, second_col, routes[:, 1:2], 1)
    either = (first_table | second_table).astype(HALF)
    r.table[:, :count] = first_table.astype(FULL)
    r.table[:, count:] = second_table.astype(FULL)
    r.across[:count, :] = first_back.astype(HALF)
    r.across[count:, :] = second_back.astype(HALF)

    r.send_grads[...] = fast(either, r.out_grad[...]).astype(HALF)
    dispatch(1)

    step_row = softplus(r.dt[...])
    step_col = exact(eye_count, step_row, NT)
    rate = r.rate[...]
    reached = jnp.where(below, 1.0, eye_count)
    sum_col = exact(reached, step_col)
    sum_row = exact(step_row, reached, NT)
    run_col = -sum_col * rate
    decay_end = jnp.exp(run_col[count - 1 : count, :])
    decay_wide = spread_heads(decay_end)
    decay_launch(jnp.broadcast_to(decay_wide, (8, width)))
    tail_col = jnp.exp(run_col[count - 1 : count, :] - run_col) * step_col
    tail_wide = spread_heads(tail_col)
    grow_wide = spread_heads(jnp.exp(run_col))
    skip_wide = spread_heads(r.skip[...])
    sum_wide = spread_heads(sum_col)
    b_side, c_side = (r.b_proj[...], r.c_proj[...])
    forward_own(1)

    square_arrive()
    scale_row_one = lax.rsqrt(jnp.sum(r.square_all[...], axis=0) / features + EPSILON)
    scale_one = to_columns(scale_row_one)[:, 0:1]
    normed = inputs * scale_one
    r.normed[...] = normed
    state_launch(exact(b_side, tail_wide * normed))

    causal = iota((count, count), 0) >= iota((count, count), 1)
    pairing = exact(c_side, b_side, TN)
    for h in range(heads):
        fall = run_col[:, h : h + 1] + sum_row[h : h + 1, :] * rate[0:1, h : h + 1]
        table = jnp.where(causal, jnp.exp(jnp.where(causal, fall, 0.0)), 0.0)
        r.mixing[:, h * count : (h + 1) * count] = table * pairing * step_row[h : h + 1, :]
        r.stack[h * count : (h + 1) * count, :] = jnp.where(lane_head == h, normed, 0.0)
    r.local[...] = exact(r.mixing[...], r.stack[...]) + skip_wide * normed

    pass_on(1)
    decay_arrive()
    state_arrive()

    def carry(states, reverse):
        held = jnp.zeros(r.state_src.shape, FULL)
        for k in range(blocks):
            at = blocks - 1 - k if reverse else k
            reach = at > block if reverse else at < block
            held = jnp.where(reach, r.decay_all[at][0:1, :] * held + states[at].astype(FULL), held)
        return held

    state_in = carry(r.state_all, False)
    carried = grow_wide * exact(c_side, state_in, TN)
    r.carried[...] = carried
    resid = (inputs + (r.local[...] + carried)).astype(HALF)
    r.resid[...] = resid
    r.send_rows[...] = fast(either, resid).astype(HALF)
    dispatch(0)
    resid_f = resid.astype(FULL)
    eye_router = (iota((stat_rows, 128), 0) == iota((stat_rows, 128), 1) + 1).astype(FULL)
    router = r.router[...]
    router_row = exact(eye_router[:, :experts], router)
    squares = exact(ones_row[0:1], resid_f * resid_f, NT)
    stat_part = exact(router_row, resid_f, NT)
    stat_launch(jnp.where(iota((stat_rows, count), 0) == 0, squares, stat_part))
    forward_own(0)
    pass_on(0)
    for way in range(chip_count - 1):
        from_chip(1, way)
    weights[1].wait()
    weights[2].wait()
    for held in gu_s:
        held[...] = jnp.zeros_like(held)

    def chunk(d):
        for held, weight in zip(gu_s, gu_w):
            held[...] += fast(rows[:, columns(d)], weight[columns(d), :])

    chunk(place)
    relay(0)
    from_partner(0, -1)
    chunk(2 * chip + 1 - core)
    early = blocks // 2
    for k in range(1, early):
        relay(k)
    for way in range(-1, chip_count - 1):
        from_partner(1, way)
    weights[0].wait()
    cut_list = slices(units, 256)
    for n in range(max(len(cut_list), blocks - early)):
        if early + n < blocks:
            relay(early + n)
        if n < len(cut_list):
            at, span = cut_list[n]
            r.unit_raw[:, at : at + span] = fast(grads[...], down_w[at : at + span, :], NT)

    stat_arrive()
    stats = jnp.sum(r.stat_all[...], axis=0)
    scale_row = lax.rsqrt(stats[0:1] / features + EPSILON)
    raw_gap = jnp.sum(stats * hot_gap_row, axis=0, keepdims=True)
    first_weight = sigmoid(raw_gap * scale_row)
    second_weight = sigmoid(-raw_gap * scale_row)
    pick8 = iota((8, 2 * count), 0)
    slot_rows = jnp.zeros((8, 2 * count), FULL)
    for n, both in enumerate(((first_weight, second_weight), (scale_row, scale_row))):
        value = jnp.concatenate(both, axis=1)
        near = value.astype(HALF).astype(FULL)
        slot_rows = jnp.where(pick8 == 2 * n, near, slot_rows)
        slot_rows = jnp.where(pick8 == 2 * n + 1, value - near, slot_rows)
    r.slot_src[...] = jnp.zeros_like(r.slot_src)

    slot_wide = fast(slot_rows.astype(HALF), r.table[...].astype(HALF), NT)
    for e in range(blocks):
        r.slot_src[e, :, :cap] = slot_wide[:, e * cap : (e + 1) * cap]
    slot_start()
    r.slot_all[block] = r.slot_src[block]
    chunk(2 * chip_from(0) + core)
    for way in range(1, chip_count - 1):
        from_chip(0, way)
        from_partner(0, way - 1)

        def one(n):
            other = 2 * partner_chip(way - 1) + 1 - core
            chunk((1 - n) * other + n * (2 * chip_from(way) + core))

        loop(2, one)
    from_partner(0, chip_count - 2)
    chunk(2 * partner_chip(chip_count - 2) + 1 - core)

    slot_arrive()
    pick = (iota((8, 256), 0) // 2 == iota((8, 256), 1) // 128).astype(HALF)

    wides = [fast(r.slot_all[j].astype(HALF), pick, TN) for j in range(blocks)]
    for j, wide in enumerate(wides):
        r.slot_weight[j * cap : (j + 1) * cap, :] = wide[:cap, :128]
        r.slot_scale[j * cap : (j + 1) * cap, :] = wide[:cap, 128:]

    tall = 16
    r.values[...] = jnp.zeros_like(r.values)
    span = 128 if units % 128 == 0 else 64

    def some_rows(i):
        row = pl.ds(pl.multiple_of(i * tall, tall), tall)
        scale = r.slot_scale[row, :span]
        weight = r.slot_weight[row, :span]
        first = jnp.zeros((tall, span), FULL)
        second = jnp.zeros((tall, span), FULL)
        spans = range(0, units, span)
        given = [
            (
                part(gu_s, 0, row, at, span)[...],
                part(gu_s, 1, row, at, span)[...],
                r.unit_raw[row, at : at + span],
            )
            for at in spans
        ]
        found = []
        for gate_raw, up_raw, unit_raw in given:
            gate, up = (gate_raw * scale, up_raw * scale)
            sigma = sigmoid(gate)
            silu = gate * sigma
            hid = silu * up
            unit = unit_raw * weight
            gate_b = unit * up * (sigma + silu * (1.0 - sigma))
            up_b = unit * silu
            first = first + hid * unit_raw
            second = second + (gate_b * gate_raw + up_b * up_raw)
            values = (hid, hid * weight, gate_b, up_b, gate_b * scale, up_b * scale)
            found.append([value.astype(HALF) for value in values])
        for at, (hid, hid2, gate_b, up_b, gate_b2, up_b2) in zip(spans, found):
            r.hidden[row, at : at + span] = hid
            r.hidden2[row, at : at + span] = hid2
            part(gu_back, 0, row, at, span)[...] = gate_b
            part(gu_back, 1, row, at, span)[...] = up_b
            part(gu_back2, 0, row, at, span)[...] = gate_b2
            part(gu_back2, 1, row, at, span)[...] = up_b2
        r.values[row, :span] = first
        r.values[row, 128 : 128 + span] = second

    loop(total // tall, some_rows)
    def send_values():
        r.value_src[...] = jnp.zeros_like(r.value_src)
        lane_sums = (iota((8, 256), 0) == iota((8, 256), 1) // 128).astype(FULL)
        value_rows = exact(lane_sums, r.values[...], NT)
        for j in range(blocks):
            r.value_src[j, :, :cap] = value_rows[:, j * cap : (j + 1) * cap]
        value_start()
        r.value_all[block] = r.value_src[block]

    def both_columns(c):
        return pl.ds(pl.multiple_of(2 * c * width, 256), 2 * width)

    def input_term(c):
        result = None
        for back, weight in zip(gu_back, gu_w):
            term = fast(back[...], weight[both_columns(c), :], NT)
            result = term if result is None else result + term
        return result

    def output_term(c):
        return fast(r.hidden[...], down_w[:, both_columns(c)])

    wide_cut = 256

    def weight_grads(lo, hi):
        def one(i):
            at = pl.ds(pl.multiple_of(i * wide_cut, wide_cut), wide_cut)
            if fused:
                value = fast(rows[:, at], gu_back2[0][...], TN)
                r.gate_grad[at, :] = value[:, :units].astype(HALF)
                r.up_grad[at, :] = value[:, units:].astype(HALF)
            else:
                r.gate_grad[at, :] = fast(rows[:, at], gu_back2[0][...], TN).astype(HALF)
                r.up_grad[at, :] = fast(rows[:, at], gu_back2[1][...], TN).astype(HALF)

        lax.fori_loop(lo, hi, lambda i, c: (one(i), c)[1], 0)

    cuts = features // wide_cut

    tiles(1, input_term, 2, send_values)

    combine(1)
    value_arrive()
    inner_part = jnp.zeros((8, 2 * count), FULL)
    for j in range(blocks):
        inner_part = inner_part + exact(
            r.value_all[j, :, :cap], r.table[j * cap : (j + 1) * cap, :]
        )
    inner_launch(inner_part)

    tiles(0, output_term, chip_count - 1, lambda: finish(1))
    weight_grads(0, cuts // 4)
    inner_arrive()
    inner_all = jnp.sum(r.inner_all[...], axis=0)
    gap_grad = first_weight * second_weight * (inner_all[0:1, :count] - inner_all[0:1, count:])
    inner_row = inner_all[1:2, :count] + inner_all[1:2, count:] + gap_grad * raw_gap
    row8 = iota((8, count), 0)
    packed = jnp.where(row8 == 0, scale_row, 0.0)
    packed = jnp.where(row8 == 1, inner_row, packed)
    packed = jnp.where(row8 == 2, gap_grad, packed)
    packed = jnp.where(row8 == 3, first_weight, packed)
    packed = jnp.where(row8 == 4, second_weight, packed)
    packed_cols = to_columns(packed)
    scale_two, inner_col = (packed_cols[:, 0:1], packed_cols[:, 1:2])
    gap_col = packed_cols[:, 2:3]
    weight_one, weight_two = (packed_cols[:, 3:4], packed_cols[:, 4:5])
    resid_f = r.resid[...].astype(FULL)
    router_launch(exact(gap_grad * hot_gap_row, resid_f * scale_two))
    upstream = r.out_grad[...].astype(FULL)
    r.base[...] = (
        upstream
        + scale_two * exact(gap_col * (first_col - second_col), router)
        - resid_f * (scale_two * scale_two * scale_two) * (inner_col / features)
    )

    backs_arrive(1)
    moe_grad = fast(r.across[:count, :], backs[1][...])
    moe_grad = moe_grad + fast(r.across[count:, :], backs[1][...])
    resid_grad = r.base[...] + scale_two * moe_grad
    r.resid_grad[...] = resid_grad
    sgrad_launch(exact(c_side, grow_wide * resid_grad))
    combine(0)
    normed = r.normed[...]
    pairing_back = exact(b_side, c_side, TN)
    upper = iota((count, count), 0) <= iota((count, count), 1)
    step_wide = spread_heads(step_col)
    lane8 = iota((8, 128), 1)
    row128 = iota((8, 128), 0)
    rate_parts = jnp.zeros((1, 128), FULL)
    for h in range(heads):
        at = slice(h * count, (h + 1) * count)
        own = jnp.where(lane_head == h, resid_grad, 0.0)
        pull = exact(own, normed, NT) * r.mixing[:, at]
        gap = sum_col[:, h : h + 1] - sum_row[h : h + 1, :]
        found = jnp.sum(jnp.sum(pull * gap, axis=0, keepdims=True), axis=1, keepdims=True)
        rate_parts = jnp.where(lane8[0:1] == h, found, rate_parts)
        r.stack[at, :] = own
    for h in range(heads):
        at = slice(h * count, (h + 1) * count)
        rise = -(run_col[:, h : h + 1] + sum_row[h : h + 1, :] * rate[0:1, h : h + 1])
        table = jnp.where(upper, jnp.exp(jnp.where(upper, rise, 0.0)), 0.0)
        r.mixing[:, at] = table * pairing_back
    local_grad = step_wide * exact(r.mixing[...], r.stack[...]) + skip_wide * resid_grad
    skip_lanes = jnp.sum(resid_grad * normed, axis=0, keepdims=True)
    rate_lanes = jnp.sum(resid_grad * r.carried[...] * sum_wide, axis=0, keepdims=True)
    weight_grads(cuts // 4, 5 * cuts // 8)
    finish(0)

    sgrad_arrive()
    state_grad = carry(r.sgrad_all, True)
    tail_grad = tail_wide * exact(b_side, state_grad, TN)
    normed_grad = local_grad + tail_grad
    last_launch(exact(ones_row, normed_grad * inputs, NT))
    sum_end = sum_wide[count - 1 : count, :]
    rate_lanes = rate_lanes + jnp.sum(
        normed * tail_grad * (sum_end - sum_wide), axis=0, keepdims=True
    )
    rate_lanes = rate_lanes + sum_end * decay_wide * jnp.sum(
        state_grad * state_in, axis=0, keepdims=True
    )
    head_hot = (iota((width, 128), 0) // head_dim == iota((width, 128), 1)).astype(FULL)
    row_wide = iota((8, width), 0)
    lanes = jnp.where(row_wide == 0, rate_lanes, jnp.where(row_wide == 1, skip_lanes, 0.0))
    small_part = exact(lanes, head_hot)
    small_part = jnp.where(row128 == 0, -(small_part + rate_parts), small_part)
    small_launch(small_part)

    weight_grads(5 * cuts // 8, cuts)
    backs_arrive(0)
    first_out = fast(r.across[:count, :], backs[0][...])
    second_out = fast(r.across[count:, :], backs[0][...])
    r.block_out[...] = (resid_f + (weight_one * first_out + weight_two * second_out)).astype(HALF)
    router_arrive()
    router_total = jnp.sum(r.rout_all[...], axis=0)
    r.router_grad[...] = router_total[1 : 1 + experts]

    last_arrive()
    inner_one = to_columns(jnp.sum(r.last_all[...], axis=0))[:, 0:1]
    r.token_grad[...] = (
        resid_grad
        + scale_one * normed_grad
        - inputs * (scale_one * scale_one * scale_one) * (inner_one / features)
    ).astype(HALF)
    small_arrive()
    small = jnp.sum(r.small_all[...], axis=0)
    r.rate_grad[...] = small[0:1, :heads]
    r.skip_grad[...] = small[1:2, :heads]

    for sent in (
        square_sent,
        decay_sent,
        state_sent,
        stat_sent,
        inner_sent,
        sgrad_sent,
        router_sent,
        last_sent,
        small_sent,
        slot_sent,
        value_sent,
    ):
        sent()
    lead = (blocks - 1) * cap
    for t in range(2):
        for ref, send, recv in (
            (sources[t].at[:lead], r.z_send, r.z_recv.at[t, 0]),
            (wholes[t].at[:, : (chip_count - 1) * width], r.c_send, r.c_recv.at[t, 0]),
            (wholes[t].at[:, : chip_count * width], r.p_send, r.p_recv.at[t, 0]),
            (away.at[t], r.pair_send, r.pair_recv.at[t, 0]),
            (mine.at[t, 1:], r.chip_send, r.chip_recv.at[t, 0]),
            (summed.at[t, :lead], r.back_send, r.back_recv.at[t]),
        ):
            waits(ref, (send.at[t], recv))[1]()


PIECES = 4


def write_kernel(hidden, grads, *refs):
    amount = (len(refs) - 2) // 2
    ready, outs, down, sems = (refs[:amount], refs[amount:-2], refs[-2], refs[-1])
    copies = []

    def send(src, dst, rows, at):
        cut = pl.ds(at, rows)
        copies.append(pltpu.make_async_copy(src.at[cut], dst.at[cut], sems.at[len(copies)]))
        copies[-1].start()

    for src, dst in zip(ready, outs):
        rows = src.shape[0]
        pieces = PIECES if rows % (16 * PIECES) == 0 and rows >= 512 else 1
        for at in range(0, rows, rows // pieces):
            send(src, dst, rows // pieces, at)
    for at, rows in slices(down.shape[0], 256):
        down[at : at + rows, :] = fast(hidden[:, at : at + rows], grads[...], TN).astype(HALF)
        send(down, outs[-1], rows, at)
    for copy in copies:
        copy.wait()


def body(
    tokens,
    routes,
    dt_raw,
    b_proj,
    c_proj,
    decay_rate,
    skip_gain,
    router_weight,
    gate_weight,
    up_weight,
    down_weight,
    out_grad,
):
    peers, blocks = (lax.axis_size(DP), lax.axis_size(EXPERT))
    chip_count = peers // 2
    count, width = tokens.shape
    features, units = gate_weight.shape[1:]
    experts, heads, state = (router_weight.shape[1], decay_rate.shape[0], b_proj.shape[1])
    capacity = 5 * count // (2 * blocks)
    cap = -(-capacity // 16) * 16
    total = blocks * cap
    fused = units % 128 == 0
    stat_rows = -(-(1 + experts) // 8) * 8
    vmem = pl.BlockSpec(memory_space=pltpu.VMEM)
    hbm = pl.BlockSpec(memory_space=pltpu.HBM)
    dma = pltpu.SemaphoreType.DMA
    loaded = dict(
        tokens=tokens,
        routes=routes.T,
        dt=dt_raw.T,
        b_proj=b_proj.T,
        c_proj=c_proj.T,
        rate=decay_rate[None],
        skip=skip_gain[None],
        router=router_weight.T,
        out_grad=out_grad,
    )
    given = {name + HBM: array for name, array in loaded.items()}
    given.update(gate_hbm=gate_weight, up_hbm=up_weight, down_hbm=down_weight)
    made = dict(
        block_out=((count, width), HALF),
        token_grad=((count, width), HALF),
        gate_grad=((features, units), HALF),
        up_grad=((features, units), HALF),
        router_grad=((experts, width), FULL),
        rate_grad=((1, heads), FULL),
        skip_grad=((1, heads), FULL),
        hidden2=((total, units), HALF),
        grads=((total, features), HALF),
    )
    if fused:
        split = dict(
            gu_w=((features, 2 * units), HALF),
            gu_s=((total, 2 * units), FULL),
            gu_back=((total, 2 * units), HALF),
            gu_back2=((total, 2 * units), HALF),
        )
    else:
        split = dict(
            gate_w=((features, units), HALF),
            gate_s=((total, units), FULL),
            gate_back=((total, units), HALF),
            gate_back2=((total, units), HALF),
            up_w=((features, units), HALF),
            up_s=((total, units), FULL),
            up_back=((total, units), HALF),
            up_back2=((total, units), HALF),
        )
    scratch = dict(
        split,
        down_w=((units, features), HALF),
        rows=((total, features), HALF),
        send_rows=((total, width), HALF),
        send_grads=((total, width), HALF),
        back_f=((total, width), HALF),
        back_b=((total, width), HALF),
        unit_raw=((total, units), FULL),
        hidden=((total, units), HALF),
        away=((2, chip_count, total, width), HALF),
        mine=((2, chip_count, total, width), HALF),
        pair=((2, chip_count, total, width), HALF),
        chips=((2, chip_count - 1, total, width), HALF),
        summed=((2, total, width), HALF),
        held=((total, width), FULL),
        table=((total, 2 * count), FULL),
        across=((2 * count, total), HALF),
        normed=((count, width), FULL),
        local=((count, width), FULL),
        carried=((count, width), FULL),
        base=((count, width), FULL),
        resid_grad=((count, width), FULL),
        resid=((count, width), HALF),
        mixing=((count, heads * count), FULL),
        stack=((heads * count, width), FULL),
        slot_weight=((total, 128), FULL),
        slot_scale=((total, 128), FULL),
        values=((total, 256), FULL),
        slot_src=((blocks, 8, 128), FULL),
        slot_all=((blocks, 8, 128), FULL),
        value_src=((blocks, 8, 128), FULL),
        value_all=((blocks, 8, 128), FULL),
    )
    exchanged = dict(
        square=(DP, (8, count)),
        decay=(EXPERT, (8, width)),
        state=(EXPERT, (state, width)),
        stat=(DP, (stat_rows, count)),
        inner=(DP, (8, 2 * count)),
        sgrad=(EXPERT, (state, width)),
        rout=(EXPERT, (stat_rows, width)),
        last=(DP, (8, count)),
        small=(EXPERT, (8, 128)),
    )
    sems = dict(slot_sems=dma((2,)), value_sems=dma((2,)))
    for name, (axis, shape) in exchanged.items():
        kind = HALF if shape == (state, width) else FULL
        scratch[name + SRC] = (shape, kind)
        scratch[name + ALL] = ((lax.axis_size(axis),) + shape, kind)
        sems[name + SEMS] = dma((2,))
    for name, array in loaded.items():
        scratch[name] = (array.shape, array.dtype)
    shapes = dict(
        z=(2, blocks - 1),
        c=(2, chip_count - 1),
        p=(2, chip_count),
        pair=(2, chip_count),
        chip=(2, chip_count - 1),
        back=(2,),
    )
    for name, shape in shapes.items():
        sems[name + SEND] = dma((2,))
        sems[name + RECV] = dma(shape)
    sems.update(local_sem=dma((2,)), weight_sem=dma((3,)), load_sem=dma((len(loaded),)), u_recv=dma((blocks,)), piece_recv=dma((2, 2, blocks)))
    names = [*given, *made, *scratch, *sems]
    results = pl.pallas_call(
        functools.partial(step_kernel, names, list(loaded), capacity, cap, fused),
        out_shape=[jax.ShapeDtypeStruct(shape, kind) for shape, kind in made.values()],
        in_specs=[hbm] * len(given),
        out_specs=[vmem] * len(made),
        scratch_shapes=[pltpu.VMEM(shape, kind) for shape, kind in scratch.values()]
        + list(sems.values()),
        compiler_params=pltpu.CompilerParams(
            collective_id=7, has_side_effects=True, vmem_limit_bytes=40 << 20
        ),
        name="step",
    )(*[pltpu.with_memory_space_constraint(x, pltpu.HBM) for x in given.values()])
    *ready, hidden, grads = results
    shapes = [*ready, jax.ShapeDtypeStruct((units, features), HALF)]
    block_out, token_grad, gate_part, up_part, router_part, rate, skip, down_part = pl.pallas_call(
        write_kernel,
        out_shape=[jax.ShapeDtypeStruct(like.shape, like.dtype) for like in shapes],
        in_specs=[vmem] * len(results),
        out_specs=[hbm] * len(shapes),
        scratch_shapes=[pltpu.VMEM((units, features), HALF), dma((len(shapes) * PIECES,))],
        compiler_params=pltpu.CompilerParams(vmem_limit_bytes=12 << 20),
        name="write",
    )(hidden, grads, *ready)
    return (
        block_out,
        token_grad,
        gate_part[None],
        up_part[None],
        down_part[None],
        router_part.T,
        rate[0],
        skip[0],
    )


def solution(mesh):
    return jax.shard_map(
        body,
        mesh=mesh,
        in_specs=(
            P(EXPERT, DP),
            P(EXPERT, None),
            P(EXPERT, DP),
            P(EXPERT, None),
            P(EXPERT, None),
            P(DP),
            P(DP),
            P(DP, None),
            P(EXPERT, None, DP),
            P(EXPERT, None, DP),
            P(EXPERT, DP, None),
            P(EXPERT, DP),
        ),
        out_specs=(
            P(EXPERT, DP),
            P(EXPERT, DP),
            P(EXPERT, None, DP),
            P(EXPERT, None, DP),
            P(EXPERT, DP, None),
            P(DP, None),
            P(DP),
            P(DP),
        ),
        check_vma=False,
    )
```

```python
import functools
import types
import jax
import jax.numpy as jnp
from jax import lax
from jax.experimental import pallas as pl
from jax.experimental.pallas import tpu as pltpu
from jax.sharding import PartitionSpec as P


EPSILON = 1e-06
HIGHEST = lax.Precision.HIGHEST
MESH = pl.DeviceIdType.MESH
DP, EXPERT = ("dp", "expert")
SEND, RECV, SRC, ALL, SEMS, HBM = ("_send", "_recv", "_src", "_all", "_sems", "_hbm")
HALF, FULL = (jnp.bfloat16, jnp.float32)
NN = (((1,), (0,)), ((), ()))
NT = (((1,), (1,)), ((), ()))
TN = (((0,), (0,)), ((), ()))


def loop(count, step):
    def run(i, carry):
        step(i)
        return carry

    lax.fori_loop(0, count, run, 0)


def slices(total, width):
    return [(at, min(width, total - at)) for at in range(0, total, width)]


def exact(a, b, dims=NN):
    return lax.dot_general(a, b, dims, precision=HIGHEST, preferred_element_type=FULL)


def fast(a, b, dims=NN):
    return lax.dot_general(a, b, dims, preferred_element_type=FULL)


def iota(shape, axis):
    return lax.broadcasted_iota(jnp.int32, shape, axis)


def softplus(v):
    return jnp.maximum(v, 0.0) + jnp.log(1.0 + jnp.exp(-jnp.abs(v)))


def sigmoid(v):
    return 0.5 + 0.5 * jnp.tanh(0.5 * v)


def step_kernel(names, loaded, capacity, cap, fused, *refs):
    r = types.SimpleNamespace(**dict(zip(names, refs)))
    peers, place = (lax.axis_size(DP), lax.axis_index(DP))
    blocks, block = (lax.axis_size(EXPERT), lax.axis_index(EXPERT))
    chip_count = peers // 2
    chip, core = (place // 2, lax.rem(place, 2))
    partner = place + 1 - 2 * core
    count, width = r.tokens.shape
    features = width * peers
    heads = r.dt.shape[0]
    head_dim = width // heads
    experts = r.router.shape[0]
    units = r.down_w.shape[0]
    total = blocks * cap
    stat_rows = r.stat_src.shape[0]
    rows, grads = (r.rows, r.grads)
    sources, wholes = ((r.send_rows, r.send_grads), (rows, grads))
    away, mine, pair, chips = (r.away, r.mine, r.pair, r.chips)
    summed = r.summed
    backs = (r.back_f, r.back_b)
    down_w = r.down_w

    def strip(j):
        return pl.ds(pl.multiple_of(j * cap, 16), cap)

    def columns(d):
        return pl.ds(pl.multiple_of(d * width, 128), width)

    def ahead(k):
        return lax.rem(block + k, blocks)

    def origin_of(k):
        return lax.rem(block + blocks - k, blocks)

    square = chip_count == 4

    def turn(along_u, along_v):
        along_x = (1 - core) * along_u + core * along_v
        along_y = core * along_u + (1 - core) * along_v
        x = lax.rem(lax.rem(chip, 2) + along_x, 2)
        return 2 * lax.rem(chip // 2 + along_y, 2) + x

    def chip_to(way):
        if square:
            return turn((1, 0, 1)[way], (0, 1, 1)[way])
        return lax.rem(chip + way + 1, chip_count)

    def chip_from(way):
        return chip_to(way) if square else lax.rem(chip + chip_count - way - 1, chip_count)

    def partner_chip(way):
        if way < 0:
            return chip
        return chip_to((1, 0, 2)[way]) if square else chip_from(way)

    def chip_in_turn(q):
        if square:
            x = lax.rem(lax.rem(chip, 2) + 1 - q // 2, 2)
            return 2 * lax.rem(chip // 2 + 1 - lax.rem(q, 2), 2) + x
        return lax.rem(chip + q + 1, chip_count)

    if fused:
        gu_w, gu_s = ((r.gu_w,), (r.gu_s,))
        gu_back, gu_back2 = ((r.gu_back,), (r.gu_back2,))
        halves = (r.gu_w.at[:, :units], r.gu_w.at[:, units:])

        def part(group, which, row, at, span):
            lo = at + which * units
            return group[0].at[row, lo : lo + span]
    else:
        gu_w, gu_s = ((r.gate_w, r.up_w), (r.gate_s, r.up_s))
        gu_back = (r.gate_back, r.up_back)
        gu_back2 = (r.gate_back2, r.up_back2)
        halves = (r.gate_w, r.up_w)

        def part(group, which, row, at, span):
            return group[which].at[row, at : at + span]

    weights = [
        pltpu.make_async_copy(hbm.at[0], held, r.weight_sem.at[n])
        for n, (hbm, held) in enumerate(
            ((r.down_hbm, down_w), (r.gate_hbm, halves[0]), (r.up_hbm, halves[1]))
        )
    ]
    loads = {
        name: pltpu.make_async_copy(getattr(r, name + HBM), getattr(r, name), r.load_sem.at[n])
        for n, name in enumerate(loaded)
    }
    for item in loads.values():
        item.start()

    barrier = pltpu.get_barrier_semaphore()
    for axis, amount, me in ((DP, peers, place), (EXPERT, blocks, block)):

        def signal(k):
            pl.semaphore_signal(
                barrier, 1, device_id={axis: lax.rem(me + k + 1, amount)}, device_id_type=MESH
            )

        loop(amount - 1, signal)

    def waits(ref, sems):
        whole = pltpu.make_async_remote_copy(
            src_ref=ref,
            dst_ref=ref,
            send_sem=sems[0],
            recv_sem=sems[1],
            device_id={DP: partner},
            device_id_type=MESH,
        )
        return whole.wait_recv, whole.wait_send

    def exchange(axis, src, everyone, sems):
        amount, me = (peers, place) if axis == DP else (blocks, block)

        def one(k):
            to = lax.rem(me + k + 1, amount)
            pltpu.make_async_remote_copy(
                src_ref=src(to),
                dst_ref=everyone.at[me],
                send_sem=sems.at[0],
                recv_sem=sems.at[1],
                device_id={axis: to},
                device_id_type=MESH,
            ).start()

        arrive, sent = waits(everyone.at[: amount - 1], (sems.at[0], sems.at[1]))
        return lambda: loop(amount - 1, one), arrive, sent

    def shared(axis, name):
        src, everyone = (getattr(r, name + SRC), getattr(r, name + ALL))
        start, arrive, sent = exchange(axis, lambda _: src, everyone, getattr(r, name + SEMS))

        def launch(value):
            value = value.astype(src.dtype)
            src[...] = value
            start()
            everyone[place if axis == DP else block] = value

        return launch, arrive, sent

    square_launch, square_arrive, square_sent = shared(DP, "square")
    decay_launch, decay_arrive, decay_sent = shared(EXPERT, "decay")
    state_launch, state_arrive, state_sent = shared(EXPERT, "state")
    stat_launch, stat_arrive, stat_sent = shared(DP, "stat")
    inner_launch, inner_arrive, inner_sent = shared(DP, "inner")
    sgrad_launch, sgrad_arrive, sgrad_sent = shared(EXPERT, "sgrad")
    router_launch, router_arrive, router_sent = shared(EXPERT, "rout")
    last_launch, last_arrive, last_sent = shared(DP, "last")
    small_launch, small_arrive, small_sent = shared(EXPERT, "small")
    slot_start, slot_arrive, slot_sent = exchange(
        EXPERT, lambda to: r.slot_src.at[to], r.slot_all, r.slot_sems
    )
    value_start, value_arrive, value_sent = exchange(
        EXPERT, lambda to: r.value_src.at[to], r.value_all, r.value_sems
    )

    def own_copy(t):
        return pltpu.make_async_copy(
            sources[t].at[strip(block), :],
            wholes[t].at[strip(block), columns(place)],
            r.local_sem.at[t],
        )

    def z_copy(t, k, land):
        return pltpu.make_async_remote_copy(
            src_ref=sources[t].at[strip(ahead(k)), :],
            dst_ref=wholes[t].at[strip(land), columns(place)],
            send_sem=r.z_send.at[t],
            recv_sem=r.z_recv.at[t, k - 1],
            device_id={EXPERT: ahead(k)},
            device_id_type=MESH,
        )

    def spread_copy(t, k, way, owner, to):
        cut = wholes[t].at[strip(origin_of(k)), columns(owner)]
        return pltpu.make_async_remote_copy(
            src_ref=cut,
            dst_ref=cut,
            send_sem=r.c_send.at[t],
            recv_sem=r.u_recv.at[k] if (t, way) == (0, 0) else r.c_recv.at[t, way],
            device_id={DP: 2 * to + core},
            device_id_type=MESH,
        )

    def partner_copy(t, way, owner):
        cut = wholes[t].at[:, columns(owner)]
        return pltpu.make_async_remote_copy(
            src_ref=cut,
            dst_ref=cut,
            send_sem=r.p_send.at[t],
            recv_sem=r.p_recv.at[t, way + 1],
            device_id={DP: partner},
            device_id_type=MESH,
        )

    def dispatch(t):
        own_copy(t).start()
        loop(blocks - 1, lambda k: z_copy(t, k + 1, block).start())

    def forward(t, k):
        for way in range(2 if square and t == 0 else chip_count - 1):
            spread_copy(t, k, way, place, chip_to(way)).start()

    def forward_own(t):
        own_copy(t).wait()
        forward(t, 0)

    def pass_on(t):
        def one(n):
            z_copy(t, n + 1, origin_of(n + 1)).wait_recv()
            forward(t, n + 1)

        loop(blocks - 1, one)
        partner_copy(t, -1, place).start()

    def from_chip(t, way):
        owner = 2 * chip_from(way) + core
        cut = wholes[t].at[:, columns(owner)]
        waits(cut, (r.c_send.at[t], r.c_recv.at[t, way]))[0]()
        partner_copy(t, way, owner).start()

    def relay(k):
        owner = 2 * chip_from(0) + core
        spread_copy(0, k, 0, owner, chip_to(0)).wait_recv()
        if square:
            spread_copy(0, k, 2, owner, chip_to(1)).start()
        if k == blocks - 1:
            partner_copy(0, 0, owner).start()

    def from_partner(t, way):
        partner_copy(t, way, 2 * partner_chip(way) + 1 - core).wait_recv()

    def pair_copy(t, c):
        return pltpu.make_async_remote_copy(
            src_ref=away.at[t, c],
            dst_ref=pair.at[t, c],
            send_sem=r.pair_send.at[t],
            recv_sem=r.pair_recv.at[t, c],
            device_id={DP: partner},
            device_id_type=MESH,
        )

    def chip_copy(t, way, c, to):
        return pltpu.make_async_remote_copy(
            src_ref=mine.at[t, c],
            dst_ref=chips.at[t, way],
            send_sem=r.chip_send.at[t],
            recv_sem=r.chip_recv.at[t, way],
            device_id={DP: 2 * to + core},
            device_id_type=MESH,
        )

    def piece_copy(t, way, n, c, to):
        return pltpu.make_async_remote_copy(
            src_ref=mine.at[t, c, strip(ahead(n + 1))],
            dst_ref=chips.at[t, way, strip(ahead(n + 1))],
            send_sem=r.chip_send.at[t],
            recv_sem=r.piece_recv.at[t, way // 2, n],
            device_id={DP: 2 * to + core},
            device_id_type=MESH,
        )

    def back_copy(t, k, land):
        return pltpu.make_async_remote_copy(
            src_ref=summed.at[t, strip(ahead(k)), :],
            dst_ref=backs[t].at[strip(land), :],
            send_sem=r.back_send.at[t],
            recv_sem=r.back_recv.at[t],
            device_id={EXPERT: ahead(k)},
            device_id_type=MESH,
        )

    def tiles(t, term, when, between):
        def settle(c):
            pair_copy(t, c).wait_recv()
            mine[t, c] = (r.held[...] + pair[t, c].astype(FULL)).astype(HALF)

        def step(q):
            pl.when(q == when)(between)
            value = term(chip_in_turn(q))
            left, right = (value[:, :width], value[:, width:])
            away[t, chip_in_turn(q)] = jnp.where(core == 0, right, left).astype(HALF)
            pair_copy(t, chip_in_turn(q)).start()

            @pl.when(q > 0)
            def _():
                c = chip_in_turn(q - 1)
                settle(c)
                if square:

                    @pl.when(q == 1)
                    def _():
                        loop(blocks, lambda n: piece_copy(t, 0, n, c, chip_to(0)).start())

                    @pl.when(q == 2 + core)
                    def _():
                        chip_copy(t, 1, c, chip_to(0)).start()
                else:
                    chip_copy(t, q - 1, c, c).start()

            r.held[...] = jnp.where(core == 0, left, right)

        loop(chip_count, step)
        settle(chip)

    def combine(t):
        if square:
            c = chip_to(1)

            def one(n):
                piece_copy(t, 0, n, c, c).wait_recv()
                row = strip(ahead(n + 1))
                value = mine[t, c, row].astype(FULL) + chips[t, 0, row].astype(FULL)
                mine[t, c, row] = value.astype(HALF)
                piece_copy(t, 2, n, c, c).start()

            loop(blocks, one)

    def finish(t):
        wholes_in = (1,) if square else range(chip_count - 1)
        for way in wholes_in:
            chip_copy(t, way, chip, chip_to(way)).wait_recv()

        def one(n):
            row = strip(ahead(n + 1))
            value = mine[t, chip, row].astype(FULL)
            if square:
                piece_copy(t, 2, n, chip, chip).wait_recv()
            for way in range(1 if square else 0, chip_count - 1):
                value = value + chips[t, way, row].astype(FULL)
            summed[t, row] = value.astype(HALF)

            @pl.when(n < blocks - 1)
            def _():
                back_copy(t, n + 1, block).start()

        loop(blocks, one)
        backs[t][strip(block), :] = summed[t, strip(block), :]

    def backs_arrive(t):
        arrive, _ = waits(
            backs[t].at[: (blocks - 1) * cap], (r.back_send.at[t], r.back_recv.at[t])
        )
        arrive()

    for item in loads.values():
        item.wait()
    for item in weights:
        item.start()
    inputs = r.tokens[...].astype(FULL)
    lane_head = iota((1, width), 1) // head_dim

    def spread_heads(cols):
        wide = jnp.zeros((cols.shape[0], width), FULL)
        for h in range(heads):
            wide = jnp.where(lane_head == h, cols[:, h : h + 1], wide)
        return wide

    ones_row = jnp.ones((8, width), FULL)
    square_part = exact(ones_row, inputs * inputs, NT)
    eye8 = (iota((8, 128), 0) == iota((8, 128), 1)).astype(FULL)
    eye_count = (iota((count, count), 0) == iota((count, count), 1)).astype(FULL)

    def to_columns(rows8):
        return exact(rows8, eye8, TN)

    pl.semaphore_wait(barrier, peers + blocks - 2)
    square_launch(square_part)

    routes_row = r.routes[...].astype(FULL)
    routes = exact(eye_count, routes_row, NT)
    expert_row = iota((stat_rows, count), 0).astype(FULL) - 1.0
    first_row = (routes_row[0:1, :] == expert_row).astype(FULL)
    second_row = (routes_row[1:2, :] == expert_row).astype(FULL)
    hot_gap_row = first_row - second_row
    expert_col = iota((count, experts), 1).astype(FULL)
    first_col = (routes[:, 0:1] == expert_col).astype(FULL)
    second_col = (routes[:, 1:2] == expert_col).astype(FULL)
    below = iota((count, count), 0) > iota((count, count), 1)
    above = (iota((count, count), 0) < iota((count, count), 1)).astype(HALF)
    earlier_row = fast((first_row + second_row).astype(HALF), above)
    earlier_col = fast(below.astype(HALF), (first_col + second_col).astype(HALF))

    def slot_of(earlier, hot, ids, axis):
        index = jnp.sum(earlier * hot, axis=axis, keepdims=True)
        return jnp.where(index < capacity, ids * cap + index, -1.0)

    slots_down = iota((total, count), 0).astype(FULL)
    slots_across = iota((count, total), 1).astype(FULL)
    first_table = slots_down == slot_of(earlier_row, first_row, routes_row[0:1, :], 0)
    second_table = slots_down == slot_of(earlier_row, second_row, routes_row[1:2, :], 0)
    first_back = slots_across == slot_of(earlier_col, first_col, routes[:, 0:1], 1)
    second_back = slots_across == slot_of(earlier_col, second_col, routes[:, 1:2], 1)
    either = (first_table | second_table).astype(HALF)
    r.table[:, :count] = first_table.astype(FULL)
    r.table[:, count:] = second_table.astype(FULL)
    r.across[:count, :] = first_back.astype(HALF)
    r.across[count:, :] = second_back.astype(HALF)

    r.send_grads[...] = fast(either, r.out_grad[...]).astype(HALF)
    dispatch(1)

    step_row = softplus(r.dt[...])
    step_col = exact(eye_count, step_row, NT)
    rate = r.rate[...]
    reached = jnp.where(below, 1.0, eye_count)
    sum_col = exact(reached, step_col)
    sum_row = exact(step_row, reached, NT)
    run_col = -sum_col * rate
    decay_end = jnp.exp(run_col[count - 1 : count, :])
    decay_wide = spread_heads(decay_end)
    decay_launch(jnp.broadcast_to(decay_wide, (8, width)))
    tail_col = jnp.exp(run_col[count - 1 : count, :] - run_col) * step_col
    tail_wide = spread_heads(tail_col)
    grow_wide = spread_heads(jnp.exp(run_col))
    skip_wide = spread_heads(r.skip[...])
    sum_wide = spread_heads(sum_col)
    b_side, c_side = (r.b_proj[...], r.c_proj[...])
    forward_own(1)

    square_arrive()
    scale_row_one = lax.rsqrt(jnp.sum(r.square_all[...], axis=0) / features + EPSILON)
    scale_one = to_columns(scale_row_one)[:, 0:1]
    normed = inputs * scale_one
    r.normed[...] = normed
    state_launch(exact(b_side, tail_wide * normed))

    causal = iota((count, count), 0) >= iota((count, count), 1)
    pairing = exact(c_side, b_side, TN)
    for h in range(heads):
        fall = run_col[:, h : h + 1] + sum_row[h : h + 1, :] * rate[0:1, h : h + 1]
        table = jnp.where(causal, jnp.exp(jnp.where(causal, fall, 0.0)), 0.0)
        r.mixing[:, h * count : (h + 1) * count] = table * pairing * step_row[h : h + 1, :]
        r.stack[h * count : (h + 1) * count, :] = jnp.where(lane_head == h, normed, 0.0)
    r.local[...] = exact(r.mixing[...], r.stack[...]) + skip_wide * normed

    pass_on(1)
    decay_arrive()
    state_arrive()

    def carry(states, reverse):
        held = jnp.zeros(r.state_src.shape, FULL)
        for k in range(blocks):
            at = blocks - 1 - k if reverse else k
            reach = at > block if reverse else at < block
            held = jnp.where(reach, r.decay_all[at][0:1, :] * held + states[at].astype(FULL), held)
        return held

    state_in = carry(r.state_all, False)
    carried = grow_wide * exact(c_side, state_in, TN)
    r.carried[...] = carried
    resid = (inputs + (r.local[...] + carried)).astype(HALF)
    r.resid[...] = resid
    r.send_rows[...] = fast(either, resid).astype(HALF)
    dispatch(0)
    resid_f = resid.astype(FULL)
    eye_router = (iota((stat_rows, 128), 0) == iota((stat_rows, 128), 1) + 1).astype(FULL)
    router = r.router[...]
    router_row = exact(eye_router[:, :experts], router)
    squares = exact(ones_row[0:1], resid_f * resid_f, NT)
    stat_part = exact(router_row, resid_f, NT)
    stat_launch(jnp.where(iota((stat_rows, count), 0) == 0, squares, stat_part))
    forward_own(0)
    pass_on(0)
    for way in range(chip_count - 1):
        from_chip(1, way)
    weights[1].wait()
    weights[2].wait()
    for held in gu_s:
        held[...] = jnp.zeros_like(held)

    def chunk(d):
        for held, weight in zip(gu_s, gu_w):
            held[...] += fast(rows[:, columns(d)], weight[columns(d), :])

    chunk(place)
    relay(0)
    from_partner(0, -1)
    chunk(2 * chip + 1 - core)
    stat_arrive()
    stats = jnp.sum(r.stat_all[...], axis=0)
    scale_row = lax.rsqrt(stats[0:1] / features + EPSILON)
    raw_gap = jnp.sum(stats * hot_gap_row, axis=0, keepdims=True)
    first_weight = sigmoid(raw_gap * scale_row)
    second_weight = sigmoid(-raw_gap * scale_row)
    pick8 = iota((8, 2 * count), 0)
    slot_rows = jnp.zeros((8, 2 * count), FULL)
    for n, both in enumerate(((first_weight, second_weight), (scale_row, scale_row))):
        value = jnp.concatenate(both, axis=1)
        near = value.astype(HALF).astype(FULL)
        slot_rows = jnp.where(pick8 == 2 * n, near, slot_rows)
        slot_rows = jnp.where(pick8 == 2 * n + 1, value - near, slot_rows)
    r.slot_src[...] = jnp.zeros_like(r.slot_src)

    slot_wide = fast(slot_rows.astype(HALF), r.table[...].astype(HALF), NT)
    for e in range(blocks):
        r.slot_src[e, :, :cap] = slot_wide[:, e * cap : (e + 1) * cap]
    slot_start()
    r.slot_all[block] = r.slot_src[block]
    early = blocks // 2
    for k in range(1, early):
        relay(k)
    for way in range(-1, chip_count - 1):
        from_partner(1, way)
    weights[0].wait()
    cut_list = slices(units, 256)
    for n in range(max(len(cut_list), blocks - early)):
        if early + n < blocks:
            relay(early + n)
        if n < len(cut_list):
            at, span = cut_list[n]
            r.unit_raw[:, at : at + span] = fast(grads[...], down_w[at : at + span, :], NT)

    def take_slots():
        slot_arrive()
        pick = (iota((8, 256), 0) // 2 == iota((8, 256), 1) // 128).astype(HALF)

        wides = [fast(r.slot_all[j].astype(HALF), pick, TN) for j in range(blocks)]
        for j, wide in enumerate(wides):
            r.slot_weight[j * cap : (j + 1) * cap, :] = wide[:cap, :128]
            r.slot_scale[j * cap : (j + 1) * cap, :] = wide[:cap, 128:]

    chunk(2 * chip_from(0) + core)
    for way in range(1, chip_count - 1):
        if way == chip_count - 2:
            take_slots()
        from_chip(0, way)
        from_partner(0, way - 1)

        def one(n):
            other = 2 * partner_chip(way - 1) + 1 - core
            chunk((1 - n) * other + n * (2 * chip_from(way) + core))

        loop(2, one)
    from_partner(0, chip_count - 2)
    chunk(2 * partner_chip(chip_count - 2) + 1 - core)

    tall = 16
    r.values[...] = jnp.zeros_like(r.values)
    span = 128 if units % 128 == 0 else 64

    def some_rows(i):
        row = pl.ds(pl.multiple_of(i * tall, tall), tall)
        scale = r.slot_scale[row, :span]
        weight = r.slot_weight[row, :span]
        first = jnp.zeros((tall, span), FULL)
        second = jnp.zeros((tall, span), FULL)
        spans = range(0, units, span)
        given = [
            (
                part(gu_s, 0, row, at, span)[...],
                part(gu_s, 1, row, at, span)[...],
                r.unit_raw[row, at : at + span],
            )
            for at in spans
        ]
        found = []
        for gate_raw, up_raw, unit_raw in given:
            gate, up = (gate_raw * scale, up_raw * scale)
            sigma = sigmoid(gate)
            silu = gate * sigma
            hid = silu * up
            unit = unit_raw * weight
            gate_b = unit * up * (sigma + silu * (1.0 - sigma))
            up_b = unit * silu
            first = first + hid * unit_raw
            second = second + (gate_b * gate_raw + up_b * up_raw)
            values = (hid, hid * weight, gate_b, up_b, gate_b * scale, up_b * scale)
            found.append([value.astype(HALF) for value in values])
        for at, (hid, hid2, gate_b, up_b, gate_b2, up_b2) in zip(spans, found):
            r.hidden[row, at : at + span] = hid
            r.hidden2[row, at : at + span] = hid2
            part(gu_back, 0, row, at, span)[...] = gate_b
            part(gu_back, 1, row, at, span)[...] = up_b
            part(gu_back2, 0, row, at, span)[...] = gate_b2
            part(gu_back2, 1, row, at, span)[...] = up_b2
        r.values[row, :span] = first
        r.values[row, 128 : 128 + span] = second

    loop(total // tall, some_rows)
    def send_values():
        r.value_src[...] = jnp.zeros_like(r.value_src)
        lane_sums = (iota((8, 256), 0) == iota((8, 256), 1) // 128).astype(FULL)
        value_rows = exact(lane_sums, r.values[...], NT)
        for j in range(blocks):
            r.value_src[j, :, :cap] = value_rows[:, j * cap : (j + 1) * cap]
        value_start()
        r.value_all[block] = r.value_src[block]

    def both_columns(c):
        return pl.ds(pl.multiple_of(2 * c * width, 256), 2 * width)

    def input_term(c):
        result = None
        for back, weight in zip(gu_back, gu_w):
            term = fast(back[...], weight[both_columns(c), :], NT)
            result = term if result is None else result + term
        return result

    def output_term(c):
        return fast(r.hidden[...], down_w[:, both_columns(c)])

    wide_cut = 256

    def weight_grads(lo, hi):
        def one(i):
            at = pl.ds(pl.multiple_of(i * wide_cut, wide_cut), wide_cut)
            if fused:
                value = fast(rows[:, at], gu_back2[0][...], TN)
                r.gate_grad[at, :] = value[:, :units].astype(HALF)
                r.up_grad[at, :] = value[:, units:].astype(HALF)
            else:
                r.gate_grad[at, :] = fast(rows[:, at], gu_back2[0][...], TN).astype(HALF)
                r.up_grad[at, :] = fast(rows[:, at], gu_back2[1][...], TN).astype(HALF)

        lax.fori_loop(lo, hi, lambda i, c: (one(i), c)[1], 0)

    cuts = features // wide_cut

    tiles(1, input_term, 2, send_values)

    combine(1)
    value_arrive()
    inner_part = jnp.zeros((8, 2 * count), FULL)
    for j in range(blocks):
        inner_part = inner_part + exact(
            r.value_all[j, :, :cap], r.table[j * cap : (j + 1) * cap, :]
        )
    inner_launch(inner_part)

    tiles(0, output_term, chip_count - 1, lambda: finish(1))
    weight_grads(0, cuts // 4)
    inner_arrive()
    inner_all = jnp.sum(r.inner_all[...], axis=0)
    gap_grad = first_weight * second_weight * (inner_all[0:1, :count] - inner_all[0:1, count:])
    inner_row = inner_all[1:2, :count] + inner_all[1:2, count:] + gap_grad * raw_gap
    row8 = iota((8, count), 0)
    packed = jnp.where(row8 == 0, scale_row, 0.0)
    packed = jnp.where(row8 == 1, inner_row, packed)
    packed = jnp.where(row8 == 2, gap_grad, packed)
    packed = jnp.where(row8 == 3, first_weight, packed)
    packed = jnp.where(row8 == 4, second_weight, packed)
    packed_cols = to_columns(packed)
    scale_two, inner_col = (packed_cols[:, 0:1], packed_cols[:, 1:2])
    gap_col = packed_cols[:, 2:3]
    weight_one, weight_two = (packed_cols[:, 3:4], packed_cols[:, 4:5])
    resid_f = r.resid[...].astype(FULL)
    router_launch(exact(gap_grad * hot_gap_row, resid_f * scale_two))
    upstream = r.out_grad[...].astype(FULL)
    r.base[...] = (
        upstream
        + scale_two * exact(gap_col * (first_col - second_col), router)
        - resid_f * (scale_two * scale_two * scale_two) * (inner_col / features)
    )

    backs_arrive(1)
    moe_grad = fast(r.across[:count, :], backs[1][...])
    moe_grad = moe_grad + fast(r.across[count:, :], backs[1][...])
    resid_grad = r.base[...] + scale_two * moe_grad
    r.resid_grad[...] = resid_grad
    sgrad_launch(exact(c_side, grow_wide * resid_grad))
    combine(0)
    normed = r.normed[...]
    pairing_back = exact(b_side, c_side, TN)
    upper = iota((count, count), 0) <= iota((count, count), 1)
    step_wide = spread_heads(step_col)
    lane8 = iota((8, 128), 1)
    row128 = iota((8, 128), 0)
    rate_parts = jnp.zeros((1, 128), FULL)
    for h in range(heads):
        at = slice(h * count, (h + 1) * count)
        own = jnp.where(lane_head == h, resid_grad, 0.0)
        pull = exact(own, normed, NT) * r.mixing[:, at]
        gap = sum_col[:, h : h + 1] - sum_row[h : h + 1, :]
        found = jnp.sum(jnp.sum(pull * gap, axis=0, keepdims=True), axis=1, keepdims=True)
        rate_parts = jnp.where(lane8[0:1] == h, found, rate_parts)
        r.stack[at, :] = own
    for h in range(heads):
        at = slice(h * count, (h + 1) * count)
        rise = -(run_col[:, h : h + 1] + sum_row[h : h + 1, :] * rate[0:1, h : h + 1])
        table = jnp.where(upper, jnp.exp(jnp.where(upper, rise, 0.0)), 0.0)
        r.mixing[:, at] = table * pairing_back
    local_grad = step_wide * exact(r.mixing[...], r.stack[...]) + skip_wide * resid_grad
    skip_lanes = jnp.sum(resid_grad * normed, axis=0, keepdims=True)
    rate_lanes = jnp.sum(resid_grad * r.carried[...] * sum_wide, axis=0, keepdims=True)
    weight_grads(cuts // 4, 5 * cuts // 8)
    finish(0)

    sgrad_arrive()
    state_grad = carry(r.sgrad_all, True)
    tail_grad = tail_wide * exact(b_side, state_grad, TN)
    normed_grad = local_grad + tail_grad
    last_launch(exact(ones_row, normed_grad * inputs, NT))
    sum_end = sum_wide[count - 1 : count, :]
    rate_lanes = rate_lanes + jnp.sum(
        normed * tail_grad * (sum_end - sum_wide), axis=0, keepdims=True
    )
    rate_lanes = rate_lanes + sum_end * decay_wide * jnp.sum(
        state_grad * state_in, axis=0, keepdims=True
    )
    head_hot = (iota((width, 128), 0) // head_dim == iota((width, 128), 1)).astype(FULL)
    row_wide = iota((8, width), 0)
    lanes = jnp.where(row_wide == 0, rate_lanes, jnp.where(row_wide == 1, skip_lanes, 0.0))
    small_part = exact(lanes, head_hot)
    small_part = jnp.where(row128 == 0, -(small_part + rate_parts), small_part)
    small_launch(small_part)

    weight_grads(5 * cuts // 8, cuts)
    backs_arrive(0)
    first_out = fast(r.across[:count, :], backs[0][...])
    second_out = fast(r.across[count:, :], backs[0][...])
    r.block_out[...] = (resid_f + (weight_one * first_out + weight_two * second_out)).astype(HALF)
    router_arrive()
    router_total = jnp.sum(r.rout_all[...], axis=0)
    r.router_grad[...] = router_total[1 : 1 + experts]

    last_arrive()
    inner_one = to_columns(jnp.sum(r.last_all[...], axis=0))[:, 0:1]
    r.token_grad[...] = (
        resid_grad
        + scale_one * normed_grad
        - inputs * (scale_one * scale_one * scale_one) * (inner_one / features)
    ).astype(HALF)
    small_arrive()
    small = jnp.sum(r.small_all[...], axis=0)
    r.rate_grad[...] = small[0:1, :heads]
    r.skip_grad[...] = small[1:2, :heads]

    for sent in (
        square_sent,
        decay_sent,
        state_sent,
        stat_sent,
        inner_sent,
        sgrad_sent,
        router_sent,
        last_sent,
        small_sent,
        slot_sent,
        value_sent,
    ):
        sent()
    lead = (blocks - 1) * cap
    for t in range(2):
        for ref, send, recv in (
            (sources[t].at[:lead], r.z_send, r.z_recv.at[t, 0]),
            (wholes[t].at[:, : (chip_count - 1) * width], r.c_send, r.c_recv.at[t, 0]),
            (wholes[t].at[:, : chip_count * width], r.p_send, r.p_recv.at[t, 0]),
            (away.at[t], r.pair_send, r.pair_recv.at[t, 0]),
            (mine.at[t, 1:], r.chip_send, r.chip_recv.at[t, 0]),
            (summed.at[t, :lead], r.back_send, r.back_recv.at[t]),
        ):
            waits(ref, (send.at[t], recv))[1]()


PIECES = 4


def write_kernel(hidden, grads, *refs):
    amount = (len(refs) - 2) // 2
    ready, outs, down, sems = (refs[:amount], refs[amount:-2], refs[-2], refs[-1])
    copies = []

    def send(src, dst, rows, at):
        cut = pl.ds(at, rows)
        copies.append(pltpu.make_async_copy(src.at[cut], dst.at[cut], sems.at[len(copies)]))
        copies[-1].start()

    for src, dst in zip(ready, outs):
        rows = src.shape[0]
        pieces = PIECES if rows % (16 * PIECES) == 0 and rows >= 512 else 1
        for at in range(0, rows, rows // pieces):
            send(src, dst, rows // pieces, at)
    for at, rows in slices(down.shape[0], 256):
        down[at : at + rows, :] = fast(hidden[:, at : at + rows], grads[...], TN).astype(HALF)
        send(down, outs[-1], rows, at)
    for copy in copies:
        copy.wait()


def body(
    tokens,
    routes,
    dt_raw,
    b_proj,
    c_proj,
    decay_rate,
    skip_gain,
    router_weight,
    gate_weight,
    up_weight,
    down_weight,
    out_grad,
):
    peers, blocks = (lax.axis_size(DP), lax.axis_size(EXPERT))
    chip_count = peers // 2
    count, width = tokens.shape
    features, units = gate_weight.shape[1:]
    experts, heads, state = (router_weight.shape[1], decay_rate.shape[0], b_proj.shape[1])
    capacity = 5 * count // (2 * blocks)
    cap = -(-capacity // 16) * 16
    total = blocks * cap
    fused = units % 128 == 0
    stat_rows = -(-(1 + experts) // 8) * 8
    vmem = pl.BlockSpec(memory_space=pltpu.VMEM)
    hbm = pl.BlockSpec(memory_space=pltpu.HBM)
    dma = pltpu.SemaphoreType.DMA
    loaded = dict(
        tokens=tokens,
        routes=routes.T,
        dt=dt_raw.T,
        b_proj=b_proj.T,
        c_proj=c_proj.T,
        rate=decay_rate[None],
        skip=skip_gain[None],
        router=router_weight.T,
        out_grad=out_grad,
    )
    given = {name + HBM: array for name, array in loaded.items()}
    given.update(gate_hbm=gate_weight, up_hbm=up_weight, down_hbm=down_weight)
    made = dict(
        block_out=((count, width), HALF),
        token_grad=((count, width), HALF),
        gate_grad=((features, units), HALF),
        up_grad=((features, units), HALF),
        router_grad=((experts, width), FULL),
        rate_grad=((1, heads), FULL),
        skip_grad=((1, heads), FULL),
        hidden2=((total, units), HALF),
        grads=((total, features), HALF),
    )
    if fused:
        split = dict(
            gu_w=((features, 2 * units), HALF),
            gu_s=((total, 2 * units), FULL),
            gu_back=((total, 2 * units), HALF),
            gu_back2=((total, 2 * units), HALF),
        )
    else:
        split = dict(
            gate_w=((features, units), HALF),
            gate_s=((total, units), FULL),
            gate_back=((total, units), HALF),
            gate_back2=((total, units), HALF),
            up_w=((features, units), HALF),
            up_s=((total, units), FULL),
            up_back=((total, units), HALF),
            up_back2=((total, units), HALF),
        )
    scratch = dict(
        split,
        down_w=((units, features), HALF),
        rows=((total, features), HALF),
        send_rows=((total, width), HALF),
        send_grads=((total, width), HALF),
        back_f=((total, width), HALF),
        back_b=((total, width), HALF),
        unit_raw=((total, units), FULL),
        hidden=((total, units), HALF),
        away=((2, chip_count, total, width), HALF),
        mine=((2, chip_count, total, width), HALF),
        pair=((2, chip_count, total, width), HALF),
        chips=((2, chip_count - 1, total, width), HALF),
        summed=((2, total, width), HALF),
        held=((total, width), FULL),
        table=((total, 2 * count), FULL),
        across=((2 * count, total), HALF),
        normed=((count, width), FULL),
        local=((count, width), FULL),
        carried=((count, width), FULL),
        base=((count, width), FULL),
        resid_grad=((count, width), FULL),
        resid=((count, width), HALF),
        mixing=((count, heads * count), FULL),
        stack=((heads * count, width), FULL),
        slot_weight=((total, 128), FULL),
        slot_scale=((total, 128), FULL),
        values=((total, 256), FULL),
        slot_src=((blocks, 8, 128), FULL),
        slot_all=((blocks, 8, 128), FULL),
        value_src=((blocks, 8, 128), FULL),
        value_all=((blocks, 8, 128), FULL),
    )
    exchanged = dict(
        square=(DP, (8, count)),
        decay=(EXPERT, (8, width)),
        state=(EXPERT, (state, width)),
        stat=(DP, (stat_rows, count)),
        inner=(DP, (8, 2 * count)),
        sgrad=(EXPERT, (state, width)),
        rout=(EXPERT, (stat_rows, width)),
        last=(DP, (8, count)),
        small=(EXPERT, (8, 128)),
    )
    sems = dict(slot_sems=dma((2,)), value_sems=dma((2,)))
    for name, (axis, shape) in exchanged.items():
        kind = HALF if shape == (state, width) else FULL
        scratch[name + SRC] = (shape, kind)
        scratch[name + ALL] = ((lax.axis_size(axis),) + shape, kind)
        sems[name + SEMS] = dma((2,))
    for name, array in loaded.items():
        scratch[name] = (array.shape, array.dtype)
    shapes = dict(
        z=(2, blocks - 1),
        c=(2, chip_count - 1),
        p=(2, chip_count),
        pair=(2, chip_count),
        chip=(2, chip_count - 1),
        back=(2,),
    )
    for name, shape in shapes.items():
        sems[name + SEND] = dma((2,))
        sems[name + RECV] = dma(shape)
    sems.update(local_sem=dma((2,)), weight_sem=dma((3,)), load_sem=dma((len(loaded),)), u_recv=dma((blocks,)), piece_recv=dma((2, 2, blocks)))
    names = [*given, *made, *scratch, *sems]
    results = pl.pallas_call(
        functools.partial(step_kernel, names, list(loaded), capacity, cap, fused),
        out_shape=[jax.ShapeDtypeStruct(shape, kind) for shape, kind in made.values()],
        in_specs=[hbm] * len(given),
        out_specs=[vmem] * len(made),
        scratch_shapes=[pltpu.VMEM(shape, kind) for shape, kind in scratch.values()]
        + list(sems.values()),
        compiler_params=pltpu.CompilerParams(
            collective_id=7, has_side_effects=True, vmem_limit_bytes=40 << 20
        ),
        name="step",
    )(*[pltpu.with_memory_space_constraint(x, pltpu.HBM) for x in given.values()])
    *ready, hidden, grads = results
    shapes = [*ready, jax.ShapeDtypeStruct((units, features), HALF)]
    block_out, token_grad, gate_part, up_part, router_part, rate, skip, down_part = pl.pallas_call(
        write_kernel,
        out_shape=[jax.ShapeDtypeStruct(like.shape, like.dtype) for like in shapes],
        in_specs=[vmem] * len(results),
        out_specs=[hbm] * len(shapes),
        scratch_shapes=[pltpu.VMEM((units, features), HALF), dma((len(shapes) * PIECES,))],
        compiler_params=pltpu.CompilerParams(vmem_limit_bytes=12 << 20),
        name="write",
    )(hidden, grads, *ready)
    return (
        block_out,
        token_grad,
        gate_part[None],
        up_part[None],
        down_part[None],
        router_part.T,
        rate[0],
        skip[0],
    )


def solution(mesh):
    return jax.shard_map(
        body,
        mesh=mesh,
        in_specs=(
            P(EXPERT, DP),
            P(EXPERT, None),
            P(EXPERT, DP),
            P(EXPERT, None),
            P(EXPERT, None),
            P(DP),
            P(DP),
            P(DP, None),
            P(EXPERT, None, DP),
            P(EXPERT, None, DP),
            P(EXPERT, DP, None),
            P(EXPERT, DP),
        ),
        out_specs=(
            P(EXPERT, DP),
            P(EXPERT, DP),
            P(EXPERT, None, DP),
            P(EXPERT, None, DP),
            P(EXPERT, DP, None),
            P(DP, None),
            P(DP),
            P(DP),
        ),
        check_vma=False,
    )
```
